128 devices in a mesh: batch: 16 (over y, x), tile: 8 (over z, core).
Axes of the slice: x: 4, y: 4, z: 4, core: 2. Of those that a mesh axis runs over, the one named last changes fastest.
Arguments:
- object_field: float32 [2, 2, 6144, 3072], P(None, None, 'batch', 'tile'), may hold values from -6 to 6
- probe_wave: bfloat16 [2, 256, 256], replicated, may hold values from -4.1875 to 4.1875
- intensities: float32 [2048, 256, 256], P(('batch', 'tile')), may hold values from 0 to 4
- owner_rows: int32 [2048, 1], P(('batch', 'tile')), may hold values from 0 to 15; in each aligned block of 16 rows (0 to 15, 16 to 31, ...) at most 2 rows name the same one
- offsets: int32 [2048, 2], P(('batch', 'tile')), may hold values from 0 to 128
Outputs:
- new_object: float32 [2, 2, 6144, 3072], P(None, None, 'batch', 'tile')
- new_probe: float32 [2, 256, 256], replicated
The draws below stay inside these ranges and needn't reach their ends.
Inputs may be any that keep to these rules, and one draw needn't show every extreme that they name: `owner_rows`: within the 16 positions of one device, each tile row is named at most 2 times.
All inputs are finite; a program needn't handle non-finite values.
Results may differ from the reference program's by a relative error of at most 0.008.
The reference program's roundings to bfloat16 on the way count: a program that leaves them out, or rounds other values in their place, can miss the bound.
Values may be sent and summed in bfloat16 or wider, within the bound.
No kernel may reach another device: no remote copies, remote signals or barrier semaphores. Data moves between devices by JAX's collectives and lax.ppermute only.
A program may use at most 192 MiB of HBM per device.

```python
import math
import jax
import jax.numpy as jnp
import numpy as np
from jax import lax

W = 256
S = 2
TS = 384
P_DEV = 16
CAP = 2
POSITIONS = 2048
NY = 6144
NX = 3072
N_BATCH = 16
N_TILE = 8


def set_ends(result, rng, least, largest):
    spot = [jax.random.randint(jax.random.fold_in(rng, axis), (), 0, length) for axis, length in enumerate(result.shape)]
    main_axis = result.shape.index(max(result.shape))
    neighbour = spot[:main_axis] + [(spot[main_axis] + 1) % result.shape[main_axis]] + spot[main_axis + 1:]
    return result.at[tuple(spot)].set(least).at[tuple(neighbour)].set(largest)


def shard_levels(rng, dims, cuts, least, top_value):
    def one(dim, shards_of):
        draws = jax.random.uniform(jax.random.fold_in(jax.random.fold_in(rng, 6), dim), (shards_of,), jnp.float32, least / len(cuts), top_value / len(cuts))
        return jnp.repeat(jnp.exp(draws), dims[dim] // shards_of).reshape((-1,) + (1,) * (len(dims) - dim - 1))

    level = one(*cuts[0])
    for cut in cuts[1:]:
        level = level * one(*cut)
    return level


def assign_block(own_key, own, number, rows, count, top, limit, skew):
    sequence = jax.random.permutation(own_key, count)
    packed, usual = load_shares(count, rows * top, limit, skew, True), load_shares(count, rows * top, limit, skew, False)
    places = jnp.arange(count)

    def named(lengths, rotation):
        used = int((lengths > 0).sum())
        fixed = max(1, used // 4)
        shifted = fixed + (places - fixed + rotation * (used - fixed)) % max(1, count - fixed)
        return jnp.zeros((count,), jnp.int32).at[sequence[jnp.where(places < fixed, places, shifted)]].set(jnp.asarray(lengths, jnp.int32))

    lengths = jnp.where(number % 4 == 0, named(packed, number // 4), named(usual, number - number // 4 - 1))
    mixed = jax.random.permutation(jax.random.fold_in(own, 3), count)
    giver, sink = mixed[0:count // 2 * 2:2], mixed[1:count // 2 * 2:2]
    room = jnp.minimum(lengths[giver] - 1, limit - lengths[sink]) // 2
    room = jnp.where((giver == sequence[0]) | (sink == sequence[0]) | (lengths[sink] == 0), 0, jnp.maximum(room, 0))
    shifted = jax.random.randint(jax.random.fold_in(own, 4), (count // 2,), 0, 1 << 20) % (room + 1)
    lengths = lengths.at[giver].add(-shifted).at[sink].add(shifted)
    members = jnp.searchsorted(jnp.cumsum(lengths), jnp.arange(rows * top), side="right").astype(jnp.int32)
    grid = members.reshape(top, rows).T
    grid = grid[jax.random.permutation(jax.random.fold_in(own, 1), rows)]
    rotation = jax.random.randint(jax.random.fold_in(own, 2), (rows, 1), 0, top)
    return jnp.take_along_axis(grid, (jnp.arange(top)[None, :] + rotation) % top, axis=1)


def load_shares(number_of, total, bound, slope, full):
    portions = [(1 << 20) // math.isqrt(standing ** slope) + 1 for standing in range(1, number_of + 1)]
    largest = bound if full else min(bound, max(-(-total // number_of), total * portions[0] // sum(portions)))
    least = 1 if total - largest >= number_of - 1 else 0
    given, spare = [largest] + [least] * (number_of - 1), total - largest - least * (number_of - 1)
    while spare > 0:
        free = [i for i in range(1, number_of) if given[i] < largest] or [i for i in range(1, number_of) if given[i] < bound]
        pool, remaining = sum([portions[i] for i in free]), spare
        for i in free:
            addition = min(bound - given[i], max(1, remaining * portions[i] // pool), spare)
            given[i] = given[i] + addition
            spare = spare - addition
    return np.array(given)


def normal_values(key, dims, scale, reach, cuts=(), held_as=jnp.bfloat16):
    drawn = jax.random.normal(key, dims, jnp.float32) * scale
    if len(cuts) > 0:
        drawn = shard_levels(key, dims, cuts, -0.22, 0.18) * drawn
    return jnp.clip(drawn, min=-reach, max=reach).astype(held_as)


def setup_inputs(seed: int = 0) -> dict:
    streams_of = jax.random.split(jax.random.key(seed), 6)
    object_field = normal_values(streams_of[0], (S, 2, NY, NX), 1.0, 6.0, ((2, 16), (3, 8)), jnp.float32)
    probe_wave = normal_values(streams_of[1], (2, W, W), 0.7, 4.1875)
    intensities = jnp.clip(4.0 * jax.random.uniform(streams_of[2], (POSITIONS, W, W), jnp.float32) ** shard_levels(streams_of[2], (POSITIONS, W, W), ((0, 128),), -0.2, 0.2), 0.0, 4.0)
    owner_rows_keys = jax.random.split(jax.random.fold_in(streams_of[3], 1), POSITIONS // P_DEV)
    owner_rows_turns = jax.random.permutation(jax.random.fold_in(streams_of[3], 3), POSITIONS // P_DEV)
    owner_rows = jax.vmap(lambda own, number: assign_block(jax.random.fold_in(streams_of[3], 2), own, number, P_DEV, N_BATCH, 1, CAP, 2))(owner_rows_keys, owner_rows_turns).reshape((POSITIONS, 1))
    offsets = set_ends(jax.random.randint(streams_of[4], (POSITIONS, 2), 0, TS - W + 1), jax.random.fold_in(streams_of[4], 1), 0, TS - W).astype(jnp.int32)
    return {"object_field": object_field, "probe_wave": probe_wave, "intensities": intensities, "owner_rows": owner_rows, "offsets": offsets}


update_rate = 0.1
tv_weight = 12.0
tv_smooth = 1.0
probe_rate = 0.04

def tables(extent):
    counter = jnp.arange(extent, dtype=jnp.int32)
    product = counter[:, None] * counter[None, :] % extent
    angles = product.astype(jnp.float32) * (2.0 * math.pi / extent)
    scaling = 1.0 / math.sqrt(extent)
    cos_table = (jnp.cos(angles) * scaling).astype(jnp.bfloat16)
    sin_table = (-jnp.sin(angles) * scaling).astype(jnp.bfloat16)
    frequency = (counter + extent // 2) % extent - extent // 2
    squared = (frequency * frequency).astype(jnp.float32)
    phases = -(0.5 / extent) * (squared[:, None] + squared[None, :])
    return (cos_table, sin_table, jnp.cos(phases), jnp.sin(phases))

def transform(real_part, imag_part, cos_table, sin_table):
    extent = real_part.shape[0]
    left_stack = jnp.concatenate([cos_table, sin_table], 0)
    right_stack = jnp.concatenate([real_part, imag_part], 1)
    blocks = jnp.dot(left_stack, right_stack, preferred_element_type=jnp.float32)
    mid_real = (blocks[:extent, :extent] - blocks[extent:, extent:]).astype(jnp.bfloat16)
    mid_imag = (blocks[:extent, extent:] + blocks[extent:, :extent]).astype(jnp.bfloat16)
    left_two = jnp.concatenate([mid_real, mid_imag], 0)
    right_two = jnp.concatenate([cos_table, sin_table], 1)
    second = jnp.dot(left_two, right_two, preferred_element_type=jnp.float32)
    out_real = second[:extent, :extent] - second[extent:, extent:]
    out_imag = second[:extent, extent:] + second[extent:, :extent]
    return (out_real, out_imag)

def multislice(object_patch, probe_wave, measured, cos_table, sin_table, prop_real, prop_imag):
    slices = object_patch.shape[0]
    back_sin = -sin_table
    psi_real = probe_wave[0]
    psi_imag = probe_wave[1]
    entering = []
    for slab_index in range(slices):
        trans_real = object_patch[slab_index, 0].astype(jnp.float32)
        trans_imag = object_patch[slab_index, 1].astype(jnp.float32)
        entering.append((psi_real, psi_imag))
        wave_real = psi_real.astype(jnp.float32)
        wave_imag = psi_imag.astype(jnp.float32)
        prod_real = (wave_real * trans_real - wave_imag * trans_imag).astype(jnp.bfloat16)
        prod_imag = (wave_real * trans_imag + wave_imag * trans_real).astype(jnp.bfloat16)
        if slab_index + 1 < slices:
            far_real, far_imag = transform(prod_real, prod_imag, cos_table, sin_table)
            kick_real = (prop_real * far_real - prop_imag * far_imag).astype(jnp.bfloat16)
            kick_imag = (prop_real * far_imag + prop_imag * far_real).astype(jnp.bfloat16)
            near_real, near_imag = transform(kick_real, kick_imag, cos_table, back_sin)
            psi_real = near_real.astype(jnp.bfloat16)
            psi_imag = near_imag.astype(jnp.bfloat16)
    exit_real, exit_imag = transform(prod_real, prod_imag, cos_table, sin_table)
    misfit = 0.5 * (exit_real * exit_real + exit_imag * exit_imag - measured)
    chi_real = (misfit * exit_real).astype(jnp.bfloat16)
    chi_imag = (misfit * exit_imag).astype(jnp.bfloat16)
    grad_real, grad_imag = transform(chi_real, chi_imag, cos_table, back_sin)
    object_grads = [None] * slices
    for slab_index in reversed(range(slices)):
        trans_real = object_patch[slab_index, 0].astype(jnp.float32)
        trans_imag = object_patch[slab_index, 1].astype(jnp.float32)
        wave_real = entering[slab_index][0].astype(jnp.float32)
        wave_imag = entering[slab_index][1].astype(jnp.float32)
        object_grads[slab_index] = jnp.stack([grad_real * wave_real + grad_imag * wave_imag, grad_imag * wave_real - grad_real * wave_imag])
        dpsi_real = grad_real * trans_real + grad_imag * trans_imag
        dpsi_imag = grad_imag * trans_real - grad_real * trans_imag
        if slab_index > 0:
            back_real, back_imag = transform(dpsi_real.astype(jnp.bfloat16), dpsi_imag.astype(jnp.bfloat16), cos_table, back_sin)
            turn_real = (prop_real * back_real + prop_imag * back_imag).astype(jnp.bfloat16)
            turn_imag = (prop_real * back_imag - prop_imag * back_real).astype(jnp.bfloat16)
            grad_real, grad_imag = transform(turn_real, turn_imag, cos_table, sin_table)
    patch_grad = jnp.stack(object_grads).astype(jnp.bfloat16)
    probe_grad = jnp.stack([dpsi_real, dpsi_imag])
    return (patch_grad, probe_grad)

def tv_gradient(field):
    down_diff = jnp.roll(field, -1, axis=2) - field
    right_diff = jnp.roll(field, -1, axis=3) - field
    weight = 1.0 / jnp.sqrt(lax.optimization_barrier(jnp.sum(down_diff * down_diff + right_diff * right_diff, axis=1, keepdims=True)) + tv_smooth)
    flow_down = weight * down_diff
    flow_right = weight * right_diff
    return jnp.roll(flow_down, 1, axis=2) + jnp.roll(flow_right, 1, axis=3) - flow_down - flow_right

def reference(object_field, probe_wave, intensities, owner_rows, offsets):
    cos_table, sin_table, prop_real, prop_imag = tables(W)
    total_rows = intensities.shape[0]
    serial = jnp.arange(total_rows, dtype=jnp.int32)
    columns = serial // P_DEV % N_TILE
    row_start = (owner_rows[:, 0] * TS + offsets[:, 0]).astype(jnp.int32)
    col_start = (columns * TS + offsets[:, 1]).astype(jnp.int32)
    anchor = jnp.zeros((), jnp.int32)

    def visit_one(state_in, inputs):
        field_grad, probe_total = state_in
        measured, row_at, col_at = inputs
        start = (anchor, anchor, row_at, col_at)
        object_patch = lax.dynamic_slice(object_field, start, (S, 2, W, W)).astype(jnp.bfloat16)
        patch_grad, probe_grad = multislice(object_patch, probe_wave, measured, cos_table, sin_table, prop_real, prop_imag)
        current = lax.dynamic_slice(field_grad, start, (S, 2, W, W))
        field_grad = lax.dynamic_update_slice(field_grad, current + patch_grad.astype(jnp.float32), start)
        return ((field_grad, probe_total + probe_grad), None)
    initial = (jnp.zeros(object_field.shape, jnp.float32), jnp.zeros((2, W, W), jnp.float32))
    (field_grad, probe_total), _ = lax.scan(visit_one, initial, (intensities, row_start, col_start))
    new_object = object_field - update_rate * (field_grad + tv_weight * tv_gradient(object_field))
    new_probe = probe_wave.astype(jnp.float32) - probe_rate * probe_total
    return (new_object, new_probe)
```

```python
import jax
import jax.numpy as jnp
import numpy as np
from jax import lax
from jax.experimental import pallas as pl
from jax.experimental.pallas import tpu as pltpu
from jax.sharding import Mesh
from jax.sharding import PartitionSpec as P

BATCH = ("batch_0", "batch_1")
TILE = ("tile_0", "tile_1")
BATCH_TILE = BATCH + TILE

update_rate = 0.1
tv_weight = 12.0
tv_smooth = 1.0
probe_rate = 0.04

N = 256
T = 384
CAP = 2
R = 32
PIECES = N // R
F32 = jnp.float32
BF16 = jnp.bfloat16


def tables():
    counter = np.arange(N)
    angles = (counter[:, None] * counter[None, :] % N) * (2.0 * np.pi / N)
    cos_table = (np.cos(angles) / np.sqrt(N)).astype(jnp.bfloat16)
    sin_table = (-np.sin(angles) / np.sqrt(N)).astype(jnp.bfloat16)
    freq = (counter + N // 2) % N - N // 2
    squared = (freq * freq).astype(np.float64)
    phases = -(0.5 / N) * (squared[:, None] + squared[None, :])
    prop = np.stack([np.cos(phases), np.sin(phases)]).astype(np.float32)
    return np.stack([cos_table, sin_table, -sin_table]), prop


def rows(j):
    return pl.ds(R * j, R)


def issue(acc, regs, pushes, lhs):
    for step in range(2):
        for q in range(2):
            pltpu.matmul_push_rhs(pushes[q][step], staging_register=regs[step], mxu_index=q)
        for j in range(PIECES):
            for q in range(2):
                pltpu.matmul_acc_lhs(
                    acc[q][j], lhs[q][step](j), load_staged_rhs=regs[step] if j == 0 else None
                )


def multislice_steps(env, start, scale, slot_index, acc, x, y, psi, trans, field):
    tile, probe, ints, tab, prop, probe_sum = env
    row, col = start
    regs = (0, 1)
    lane = lax.broadcasted_iota(jnp.int32, (R, 128), 1)
    back = (128 - col) & 127
    forth = col & 127
    keep = lane < 128 - col
    moved = lane >= col

    def left(forward):
        sin, neg = (1, 2) if forward else (2, 1)
        xr, xi = x[0], x[1]
        issue(
            acc,
            regs,
            ((xr[...], xi[...]), (xr[...], xi[...])),
            (
                (lambda j: tab[0, rows(j)], lambda j: tab[neg, rows(j)]),
                (lambda j: tab[sin, rows(j)], lambda j: tab[0, rows(j)]),
            ),
        )

    def middle():
        for j in range(PIECES):
            for q in range(2):
                y[q][rows(j)] = pltpu.matmul_pop(acc[q][j]).astype(BF16)

    def right(forward):
        sin, neg = (1, 2) if forward else (2, 1)
        lhs = (lambda j: y[0][rows(j)], lambda j: y[1][rows(j)])
        issue(acc, regs, ((tab[0], tab[neg]), (tab[sin], tab[0])), (lhs, lhs))

    def pops(j):
        return pltpu.matmul_pop(acc[0][j]), pltpu.matmul_pop(acc[1][j])

    def cut(s, q, j):
        at = pl.ds(row + R * j, R)
        turned = [pltpu.roll(tile[s, q, k, at, :], back, 1) for k in range(3)]
        return jnp.concatenate(
            [jnp.where(keep, turned[0], turned[1]), jnp.where(keep, turned[1], turned[2])], 1
        )

    def put(s, q, j, value):
        value = value.astype(BF16).astype(F32)
        turned = [pltpu.roll(value[:, 128 * k : 128 * k + 128], forth, 1) for k in range(2)]
        parts = (
            jnp.where(moved, turned[0], 0.0),
            jnp.where(moved, turned[1], turned[0]),
            jnp.where(moved, 0.0, turned[1]),
        )
        at = pl.ds(row + R * j, R)
        for k in range(3):
            field[s, q, k, at, :] = field[s, q, k, at, :] + parts[k]

    def product(s, wave):
        for j in range(PIECES):
            tr, ti = cut(s, 0, j), cut(s, 1, j)
            trans[s, 0, rows(j)] = tr
            trans[s, 1, rows(j)] = ti
            pr, pi = wave[0, rows(j)].astype(F32), wave[1, rows(j)].astype(F32)
            x[0][rows(j)] = (pr * tr - pi * ti).astype(BF16)
            x[1][rows(j)] = (pr * ti + pi * tr).astype(BF16)

    def kick(sign):
        for j in range(PIECES):
            fr, fi = pops(j)
            hr, hi = prop[0, rows(j)], prop[1, rows(j)]
            if sign > 0:
                x[0][rows(j)] = (hr * fr - hi * fi).astype(BF16)
                x[1][rows(j)] = (hr * fi + hi * fr).astype(BF16)
            else:
                x[0][rows(j)] = (hr * fr + hi * fi).astype(BF16)
                x[1][rows(j)] = (hr * fi - hi * fr).astype(BF16)

    product(0, probe)
    yield
    left(True)
    yield
    middle()
    right(True)
    yield
    kick(1)
    left(False)
    yield
    middle()
    right(False)
    yield
    for j in range(PIECES):
        wr, wi = pops(j)
        wr, wi = wr.astype(BF16), wi.astype(BF16)
        psi[0, rows(j)] = wr
        psi[1, rows(j)] = wi
        wr, wi = wr.astype(F32), wi.astype(F32)
        tr, ti = cut(1, 0, j), cut(1, 1, j)
        trans[1, 0, rows(j)] = tr
        trans[1, 1, rows(j)] = ti
        x[0][rows(j)] = (wr * tr - wi * ti).astype(BF16)
        x[1][rows(j)] = (wr * ti + wi * tr).astype(BF16)
    left(True)
    yield
    middle()
    right(True)
    yield
    for j in range(PIECES):
        er, ei = pops(j)
        misfit = scale * (er * er + ei * ei - ints[slot_index, rows(j)].astype(F32))
        x[0][rows(j)] = (misfit * er).astype(BF16)
        x[1][rows(j)] = (misfit * ei).astype(BF16)
    left(False)
    yield
    middle()
    right(False)
    yield
    for j in range(PIECES):
        gr, gi = pops(j)
        wr, wi = psi[0, rows(j)].astype(F32), psi[1, rows(j)].astype(F32)
        tr, ti = trans[1, 0, rows(j)], trans[1, 1, rows(j)]
        x[0][rows(j)] = (gr * tr + gi * ti).astype(BF16)
        x[1][rows(j)] = (gi * tr - gr * ti).astype(BF16)
        put(1, 0, j, gr * wr + gi * wi)
        put(1, 1, j, gi * wr - gr * wi)
    left(False)
    yield
    middle()
    right(False)
    yield
    kick(-1)
    left(True)
    yield
    middle()
    right(True)
    yield
    for j in range(PIECES):
        gr, gi = pops(j)
        wr, wi = probe[0, rows(j)].astype(F32), probe[1, rows(j)].astype(F32)
        tr, ti = trans[0, 0, rows(j)], trans[0, 1, rows(j)]
        probe_sum[0, rows(j)] = probe_sum[0, rows(j)] + (gr * tr + gi * ti)
        probe_sum[1, rows(j)] = probe_sum[1, rows(j)] + (gi * tr - gr * ti)
        put(0, 0, j, gr * wr + gi * wi)
        put(0, 1, j, gi * wr - gr * wi)


def multislice_kernel(
    meta, tile_in, base, probe, ints, tab, prop, field_out, probe_sum, tile, field_a, field_b, *work
):
    xa, xb, ya, yb, psi_a, psi_b, trans_a, trans_b = work
    for s in range(2):
        for q in range(2):
            for k in range(3):
                at = pl.ds(128 * k, 128)
                tile[s, q, k] = tile_in[s, q, :, at].astype(BF16).astype(F32)
                field_a[s, q, k] = jnp.zeros((T, 128), F32)
                field_b[s, q, k] = jnp.zeros((T, 128), F32)
    probe_sum[...] = jnp.zeros((2, N, N), F32)
    count = meta[0]
    env = (tile, probe, ints, tab, prop, probe_sum)

    def body(acc_a, acc_b):
        for one in acc_a + acc_b:
            for ref in one:
                pltpu.matmul_pop(ref)

        @pl.loop(0, (count + 1) // 2)
        def _(pair):
            ia = 2 * pair
            there = ia + 1 < count
            ib = jnp.where(there, ia + 1, ia)
            sa, sb = meta[8 + 4 * ia], meta[8 + 4 * ib]
            at_a = (meta[9 + 4 * ia], meta[10 + 4 * ia])
            at_b = (meta[9 + 4 * ib], meta[10 + 4 * ib])
            steps_a = multislice_steps(
                env, at_a, F32(0.5), sa, acc_a, (xa.at[0], xa.at[1]), (ya.at[0], ya.at[1]), psi_a, trans_a, field_a
            )
            steps_b = multislice_steps(
                env,
                at_b,
                jnp.where(there, F32(0.5), F32(0.0)),
                sb,
                acc_b,
                (xb.at[0], xb.at[1]),
                (yb.at[0], yb.at[1]),
                psi_b,
                trans_b,
                field_b,
            )
            live = [steps_a, steps_b]
            while live:
                for one in list(live):
                    if next(one, 1) == 1:
                        live.remove(one)

    refs = tuple(tuple(pltpu.ACC(q)((R, N), F32) for _ in range(PIECES)) for q in range(2))
    pl.run_scoped(body, refs, refs)
    for s in range(2):
        for q in range(2):
            for k in range(3):
                at = pl.ds(128 * k, 128)
                grad = field_a[s, q, k] + field_b[s, q, k]
                field_out[s, q, :, at] = base[s, q, :, at] - update_rate * grad


def multislice_call(meta, tile, base, probe, ints):
    tab, prop = tables()
    vmem = pl.BlockSpec(memory_space=pltpu.VMEM)
    wide = pltpu.VMEM((2, 2, 3, T, 128), F32)
    small = pltpu.VMEM((2, N, N), BF16)
    return pl.pallas_call(
        multislice_kernel,
        out_shape=(jax.ShapeDtypeStruct((2, 2, T, T), F32), jax.ShapeDtypeStruct((2, N, N), F32)),
        in_specs=[pl.BlockSpec(memory_space=pltpu.SMEM)] + [vmem] * 6,
        out_specs=(vmem, vmem),
        scratch_shapes=[wide, wide, wide] + [small] * 6 + [pltpu.VMEM((2, 2, N, N), F32)] * 2,
        compiler_params=pltpu.CompilerParams(vmem_limit_bytes=60 << 20),
        name="multislice",
    )(meta, tile, base, probe, ints, tab, prop)


def pack_kernel(slots, values, out):
    out[...] = values[...].astype(BF16)


def pack_call(slots, intensities):
    count = intensities.shape[0]
    return pl.pallas_call(
        pack_kernel,
        out_shape=jax.ShapeDtypeStruct((count * CAP, N, N), BF16),
        grid_spec=pltpu.PrefetchScalarGridSpec(
            num_scalar_prefetch=1,
            grid=(count,),
            in_specs=[pl.BlockSpec((1, N, N), lambda i, slots: (i, 0, 0))],
            out_specs=pl.BlockSpec((1, N, N), lambda i, slots: (slots[i], 0, 0)),
        ),
        name="pack",
    )(slots, intensities)


def extended(x, sides, width):
    for axis, dim in sides:
        size, length = (lax.axis_size(axis), x.shape[dim])
        up = [(i, (i + 1) % size) for i in range(size)]
        down = [(j, i) for i, j in up]
        last = lax.slice_in_dim(x, length - width, length, axis=dim)
        first = lax.slice_in_dim(x, 0, width, axis=dim)
        before = lax.ppermute(last, axis, up)
        after = lax.ppermute(first, axis, down)
        x = jnp.concatenate([before, x, after], axis=dim)
    return x


def tv_local(padded):
    corner_cells = padded[:, :, :-1, :-1]
    down_diff = padded[:, :, 1:, :-1] - corner_cells
    right_diff = padded[:, :, :-1, 1:] - corner_cells
    weight = 1.0 / jnp.sqrt(
        jnp.sum(down_diff * down_diff + right_diff * right_diff, axis=1, keepdims=True) + tv_smooth
    )
    flow_down = weight * down_diff
    flow_right = weight * right_diff
    return (
        flow_down[:, :, :-1, 1:]
        + flow_right[:, :, 1:, :-1]
        - flow_down[:, :, 1:, 1:]
        - flow_right[:, :, 1:, 1:]
    )


def on_device(object_field, probe_wave, intensities, owner_rows, offsets):
    local_rows = intensities.shape[0]
    nbatch = lax.axis_size(BATCH)
    slots_all = nbatch * CAP
    targets = owner_rows[:, 0]
    serial = jnp.arange(local_rows, dtype=jnp.int32)
    earlier = (targets[:, None] == targets[None, :]) & (serial[None, :] < serial[:, None])
    slot_of = targets * CAP + jnp.sum(earlier.astype(jnp.int32), axis=1)
    hit = slot_of[:, None] == jnp.arange(slots_all, dtype=jnp.int32)[None, :]
    request = jnp.sum(jnp.where(hit[:, :, None], offsets[:, None, :] + 1, 0), axis=0)
    wanted = lax.all_to_all(
        request.reshape(nbatch, CAP * 2), BATCH, split_axis=0, concat_axis=0, tiled=True
    ).reshape(slots_all, 2)
    sent = pack_call(slot_of, intensities).reshape(nbatch, CAP, N, N)
    ints = lax.all_to_all(sent, BATCH, split_axis=0, concat_axis=0, tiled=True)
    ints = ints.reshape(slots_all, N, N)
    used = (wanted[:, 0] > 0).astype(jnp.int32)
    place = jnp.cumsum(used) - used
    order = jnp.arange(slots_all, dtype=jnp.int32)
    takes = (place[None, :] == order[:, None]) & (used[None, :] > 0)
    fields = jnp.stack([order, wanted[:, 0] - 1, wanted[:, 1] - 1, order], 1)
    listed = jnp.sum(jnp.where(takes[:, :, None], fields[None], 0), axis=1)
    head = jnp.full((8,), jnp.sum(used), jnp.int32)
    meta = jnp.concatenate([head, listed.reshape(-1)])
    padded = extended(object_field, ((BATCH, 2), (TILE, 3)), 1)
    base = object_field - (update_rate * tv_weight) * tv_local(padded)
    new_object, probe_local = multislice_call(meta, object_field, base, probe_wave, ints)
    probe_total = lax.psum(probe_local, BATCH_TILE)
    new_probe = probe_wave.astype(F32) - probe_rate * probe_total
    return (new_object, new_probe)


def solution(mesh):
    finer = Mesh(mesh.devices.reshape(4, 4, 4, 2), ("batch_0", "batch_1", "tile_0", "tile_1"))
    placed = (P(None, None, BATCH, TILE), P(), P(BATCH_TILE), P(BATCH_TILE), P(BATCH_TILE))
    return jax.shard_map(
        on_device,
        mesh=finer,
        in_specs=placed,
        out_specs=(P(None, None, BATCH, TILE), P()),
        check_vma=False,
    )
```

```python
import jax
import jax.numpy as jnp
import numpy as np
from jax import lax
from jax.experimental import pallas as pl
from jax.experimental.pallas import tpu as pltpu
from jax.sharding import Mesh
from jax.sharding import PartitionSpec as P

BATCH = ("batch_0", "batch_1")
TILE = ("tile_0", "tile_1")
BATCH_TILE = BATCH + TILE

update_rate = 0.1
tv_weight = 12.0
tv_smooth = 1.0
probe_rate = 0.04

N = 256
T = 384
CAP = 2
R = 32
PIECES = N // R
F32 = jnp.float32
BF16 = jnp.bfloat16


def tables():
    counter = np.arange(N)
    angles = (counter[:, None] * counter[None, :] % N) * (2.0 * np.pi / N)
    cos_table = (np.cos(angles) / np.sqrt(N)).astype(jnp.bfloat16)
    sin_table = (-np.sin(angles) / np.sqrt(N)).astype(jnp.bfloat16)
    freq = (counter + N // 2) % N - N // 2
    squared = (freq * freq).astype(np.float64)
    phases = -(0.5 / N) * (squared[:, None] + squared[None, :])
    prop = np.stack([np.cos(phases), np.sin(phases)]).astype(np.float32)
    return np.stack([cos_table, sin_table, -sin_table]), prop


def rows(j):
    return pl.ds(R * j, R)


def issue(acc, regs, pushes, lhs):
    for step in range(2):
        for q in range(2):
            pltpu.matmul_push_rhs(pushes[q][step], staging_register=regs[step], mxu_index=q)
        for j in range(PIECES):
            for q in range(2):
                pltpu.matmul_acc_lhs(
                    acc[q][j], lhs[q][step](j), load_staged_rhs=regs[step] if j == 0 else None
                )


def shared(start, acc, x, y, tab):
    row, col = start
    regs = (0, 1)
    lane = lax.broadcasted_iota(jnp.int32, (R, 128), 1)
    back = (128 - col) & 127
    forth = col & 127
    keep = lane < 128 - col
    moved = lane >= col

    def left(forward):
        sin, neg = (1, 2) if forward else (2, 1)
        xr, xi = x[0], x[1]
        issue(
            acc,
            regs,
            ((xr[...], xi[...]), (xr[...], xi[...])),
            (
                (lambda j: tab[0, rows(j)], lambda j: tab[neg, rows(j)]),
                (lambda j: tab[sin, rows(j)], lambda j: tab[0, rows(j)]),
            ),
        )

    def middle():
        for j in range(PIECES):
            for q in range(2):
                y[q][rows(j)] = pltpu.matmul_pop(acc[q][j]).astype(BF16)

    def right(forward):
        sin, neg = (1, 2) if forward else (2, 1)
        lhs = (lambda j: y[0][rows(j)], lambda j: y[1][rows(j)])
        issue(acc, regs, ((tab[0], tab[neg]), (tab[sin], tab[0])), (lhs, lhs))

    def pops(j):
        return pltpu.matmul_pop(acc[0][j]), pltpu.matmul_pop(acc[1][j])

    def cut(tile, s, q, j):
        at = pl.ds(row + R * j, R)
        turned = [pltpu.roll(tile[s, q, k, at, :], back, 1) for k in range(3)]
        return jnp.concatenate(
            [jnp.where(keep, turned[0], turned[1]), jnp.where(keep, turned[1], turned[2])], 1
        )

    def put(field, s, q, j, value):
        value = value.astype(BF16).astype(F32)
        turned = [pltpu.roll(value[:, 128 * k : 128 * k + 128], forth, 1) for k in range(2)]
        parts = (
            jnp.where(moved, turned[0], 0.0),
            jnp.where(moved, turned[1], turned[0]),
            jnp.where(moved, 0.0, turned[1]),
        )
        at = pl.ds(row + R * j, R)
        for k in range(3):
            field[s, q, k, at, :] = field[s, q, k, at, :] + parts[k]

    def kick(prop, sign):
        for j in range(PIECES):
            fr, fi = pops(j)
            hr, hi = prop[0, rows(j)], prop[1, rows(j)]
            if sign > 0:
                x[0][rows(j)] = (hr * fr - hi * fi).astype(BF16)
                x[1][rows(j)] = (hr * fi + hi * fr).astype(BF16)
            else:
                x[0][rows(j)] = (hr * fr + hi * fi).astype(BF16)
                x[1][rows(j)] = (hr * fi - hi * fr).astype(BF16)

    return left, middle, right, pops, cut, put, kick


def forward_steps(env, start, acc, x, y, psi, exits):
    tile, probe, tab, prop = env
    left, middle, right, pops, cut, _, kick = shared(start, acc, x, y, tab)
    for j in range(PIECES):
        tr, ti = cut(tile, 0, 0, j), cut(tile, 0, 1, j)
        pr, pi = probe[0, rows(j)].astype(F32), probe[1, rows(j)].astype(F32)
        x[0][rows(j)] = (pr * tr - pi * ti).astype(BF16)
        x[1][rows(j)] = (pr * ti + pi * tr).astype(BF16)
    left(True)
    yield
    middle()
    right(True)
    yield
    kick(prop, 1)
    left(False)
    yield
    middle()
    right(False)
    yield
    for j in range(PIECES):
        wr, wi = pops(j)
        wr, wi = wr.astype(BF16), wi.astype(BF16)
        psi[0, rows(j)] = wr
        psi[1, rows(j)] = wi
        wr, wi = wr.astype(F32), wi.astype(F32)
        tr, ti = cut(tile, 1, 0, j), cut(tile, 1, 1, j)
        x[0][rows(j)] = (wr * tr - wi * ti).astype(BF16)
        x[1][rows(j)] = (wr * ti + wi * tr).astype(BF16)
    left(True)
    yield
    middle()
    right(True)
    yield
    for j in range(PIECES):
        er, ei = pops(j)
        exits[0, rows(j)] = er
        exits[1, rows(j)] = ei


def backward_steps(env, start, scale, ints, acc, x, y, psi, exits, field):
    tile, probe, tab, prop, probe_sum = env
    left, middle, right, pops, cut, put, kick = shared(start, acc, x, y, tab)
    for j in range(PIECES):
        er, ei = exits[0, rows(j)], exits[1, rows(j)]
        misfit = scale * (er * er + ei * ei - ints[rows(j)].astype(F32))
        x[0][rows(j)] = (misfit * er).astype(BF16)
        x[1][rows(j)] = (misfit * ei).astype(BF16)
    left(False)
    yield
    middle()
    right(False)
    yield
    for j in range(PIECES):
        gr, gi = pops(j)
        wr, wi = psi[0, rows(j)].astype(F32), psi[1, rows(j)].astype(F32)
        tr, ti = cut(tile, 1, 0, j), cut(tile, 1, 1, j)
        x[0][rows(j)] = (gr * tr + gi * ti).astype(BF16)
        x[1][rows(j)] = (gi * tr - gr * ti).astype(BF16)
        put(field, 1, 0, j, gr * wr + gi * wi)
        put(field, 1, 1, j, gi * wr - gr * wi)
    left(False)
    yield
    middle()
    right(False)
    yield
    kick(prop, -1)
    left(True)
    yield
    middle()
    right(True)
    yield
    for j in range(PIECES):
        gr, gi = pops(j)
        wr, wi = probe[0, rows(j)].astype(F32), probe[1, rows(j)].astype(F32)
        tr, ti = cut(tile, 0, 0, j), cut(tile, 0, 1, j)
        probe_sum[0, rows(j)] = probe_sum[0, rows(j)] + (gr * tr + gi * ti)
        probe_sum[1, rows(j)] = probe_sum[1, rows(j)] + (gi * tr - gr * ti)
        put(field, 0, 0, j, gr * wr + gi * wi)
        put(field, 0, 1, j, gi * wr - gr * wi)


def interleave(*steps):
    live = list(steps)
    while live:
        for one in list(live):
            if next(one, 1) == 1:
                live.remove(one)


def list_used(wanted, listed, rank):
    def one(k, used):
        listed[used] = k
        return used + (wanted[2 * CAP * k + 2 * rank] > 0).astype(jnp.int32)

    return lax.fori_loop(0, SOURCES, one, jnp.int32(0))


def chosen(wanted, listed, count, pair, rank):
    there = 2 * pair + 1 < count
    slots = listed[2 * pair], listed[jnp.where(there, 2 * pair + 1, 2 * pair)]
    at = [2 * CAP * k + 2 * rank for k in slots]
    return slots, [(wanted[a] - 1, wanted[a + 1] - 1) for a in at], there


def round_tile(tile_in, tile):
    for s in range(2):
        for q in range(2):
            for k in range(3):
                tile[s, q, k] = tile_in[s, q, :, pl.ds(128 * k, 128)].astype(BF16).astype(F32)


def with_accumulators(body):
    def start(acc_a, acc_b):
        for one in acc_a + acc_b:
            for ref in one:
                pltpu.matmul_pop(ref)
        body(acc_a, acc_b)

    refs = tuple(tuple(pltpu.ACC(q)((R, N), F32) for _ in range(PIECES)) for q in range(2))
    pl.run_scoped(start, refs, refs)


def forward_kernel(rank, wanted, tile_in, probe, tab, prop, exits_out, psi_out, tile, listed, x, y, exits, psi, sems):
    round_tile(tile_in, tile)
    env = (tile, probe, tab, prop)

    def copies(b, at):
        return (
            pltpu.make_async_copy(exits.at[b], exits_out.at[at], sems.at[0, b]),
            pltpu.make_async_copy(psi.at[b], psi_out.at[at], sems.at[1, b]),
        )

    count = list_used(wanted, listed, rank)
    pairs = (count + 1) // 2

    def body(acc_a, acc_b):
        @pl.loop(0, pairs)
        def _(pair):
            b = pair % 2
            _, at, _ = chosen(wanted, listed, count, pair, rank)

            @pl.when(pair >= 2)
            def _():
                for one in copies(b, pair - 2):
                    one.wait()

            interleave(
                *[
                    forward_steps(
                        env,
                        at[i],
                        (acc_a, acc_b)[i],
                        (x.at[i, 0], x.at[i, 1]),
                        (y.at[i, 0], y.at[i, 1]),
                        psi.at[b, i],
                        exits.at[b, i],
                    )
                    for i in range(2)
                ]
            )
            for one in copies(b, pair):
                one.start()

        for late in (2, 1):

            @pl.when(pairs >= late)
            def _():
                for one in copies((pairs - late) % 2, pairs - late):
                    one.wait()

    with_accumulators(body)


def backward_kernel(rank, *refs):
    wanted, tile_in, probe, tab, prop, ints, exits_in, psi_in = refs[:8]
    refs = refs[8:]
    if rank:
        (field_in, probe_in), refs = refs[:2], refs[2:]
    field_out, probe_sum, tile, field_a, field_b, listed, x, y, exits, psi, sems = refs
    count = list_used(wanted, listed, rank)
    pairs = (count + 1) // 2

    def copies(b, at):
        return (
            pltpu.make_async_copy(exits_in.at[at], exits.at[b], sems.at[0, b]),
            pltpu.make_async_copy(psi_in.at[at], psi.at[b], sems.at[1, b]),
        )

    @pl.when(pairs > 0)
    def _():
        for one in copies(0, 0):
            one.start()

    round_tile(tile_in, tile)
    for s in range(2):
        for q in range(2):
            for k in range(3):
                at = pl.ds(128 * k, 128)
                field_a[s, q, k] = field_in[s, q, :, at] if rank else jnp.zeros((T, 128), F32)
                field_b[s, q, k] = jnp.zeros((T, 128), F32)
    probe_sum[...] = probe_in[...] if rank else jnp.zeros((2, N, N), F32)
    env = (tile, probe, tab, prop, probe_sum)

    def body(acc_a, acc_b):
        @pl.loop(0, pairs)
        def _(pair):
            b = pair % 2
            slots, at, there = chosen(wanted, listed, count, pair, rank)

            @pl.when(pair + 1 < pairs)
            def _():
                for one in copies(1 - b, pair + 1):
                    one.start()

            for one in copies(b, pair):
                one.wait()
            scales = F32(0.5), jnp.where(there, F32(0.5), F32(0.0))
            interleave(
                *[
                    backward_steps(
                        env,
                        at[i],
                        scales[i],
                        ints.at[slots[i]],
                        (acc_a, acc_b)[i],
                        (x.at[i, 0], x.at[i, 1]),
                        (y.at[i, 0], y.at[i, 1]),
                        psi.at[b, i],
                        exits.at[b, i],
                        (field_a, field_b)[i],
                    )
                    for i in range(2)
                ]
            )

    with_accumulators(body)
    for s in range(2):
        for q in range(2):
            for k in range(3):
                field_out[s, q, :, pl.ds(128 * k, 128)] = field_a[s, q, k] + field_b[s, q, k]


VMEM = pl.BlockSpec(memory_space=pltpu.VMEM)
SMEM = pl.BlockSpec(memory_space=pltpu.SMEM)
ANY = pl.BlockSpec(memory_space=pl.ANY)
SOURCES = 16
PAIRS = SOURCES // 2
WIDE = pltpu.VMEM((2, 2, 3, T, 128), F32)
PER_PAIR = [
    pltpu.VMEM((2, 2, N, N), BF16),
    pltpu.VMEM((2, 2, N, N), BF16),
    pltpu.VMEM((2, 2, 2, N, N), F32),
    pltpu.VMEM((2, 2, 2, N, N), BF16),
    pltpu.SemaphoreType.DMA((2, 2)),
]
LISTED = pltpu.SMEM((SOURCES + 1,), jnp.int32)


def params(positions, steps):
    flops = positions * steps * 2 * 8 * N**3
    return dict(
        compiler_params=pltpu.CompilerParams(vmem_limit_bytes=40 << 20),
        cost_estimate=pl.CostEstimate(flops=flops, transcendentals=0, bytes_accessed=positions << 20),
    )


def forward_call(rank, wanted, tile, probe):
    tab, prop = tables()
    return pl.pallas_call(
        lambda *refs: forward_kernel(rank, *refs),
        out_shape=(
            jax.ShapeDtypeStruct((PAIRS, 2, 2, N, N), F32),
            jax.ShapeDtypeStruct((PAIRS, 2, 2, N, N), BF16),
        ),
        in_specs=[SMEM] + [VMEM] * 4,
        out_specs=(ANY, ANY),
        scratch_shapes=[WIDE, LISTED] + PER_PAIR,
        name=f"forward_{rank}",
        **params(16, 3),
    )(wanted, tile, probe, tab, prop)


def backward_call(rank, wanted, tile, probe, ints, exits, psi, *carried):
    tab, prop = tables()
    return pl.pallas_call(
        lambda *refs: backward_kernel(rank, *refs),
        out_shape=(jax.ShapeDtypeStruct((2, 2, T, T), F32), jax.ShapeDtypeStruct((2, N, N), F32)),
        in_specs=[SMEM] + [VMEM] * 5 + [ANY, ANY] + [VMEM] * len(carried),
        out_specs=(VMEM, VMEM),
        scratch_shapes=[WIDE, WIDE, WIDE, LISTED] + PER_PAIR,
        name=f"backward_{rank}",
        **params(16, 3),
    )(wanted, tile, probe, tab, prop, ints, exits, psi, *carried)


def pack_kernel(slots, values, *outs):
    for i in range(values.shape[0]):
        slot = slots[i]
        for rank in range(CAP):

            @pl.when(slot % CAP == rank)
            def _():
                outs[rank][slot // CAP] = values[i].astype(BF16)


def pack_call(slots, intensities):
    out = jax.ShapeDtypeStruct((SOURCES, N, N), BF16)
    return pl.pallas_call(
        pack_kernel,
        out_shape=(out,) * CAP,
        in_specs=[SMEM, VMEM],
        out_specs=(VMEM,) * CAP,
        compiler_params=pltpu.CompilerParams(vmem_limit_bytes=40 << 20),
        name="pack",
    )(slots, intensities)


def extended(x, sides, width):
    for axis, dim in sides:
        size, length = (lax.axis_size(axis), x.shape[dim])
        up = [(i, (i + 1) % size) for i in range(size)]
        down = [(j, i) for i, j in up]
        last = lax.slice_in_dim(x, length - width, length, axis=dim)
        first = lax.slice_in_dim(x, 0, width, axis=dim)
        before = lax.ppermute(last, axis, up)
        after = lax.ppermute(first, axis, down)
        x = jnp.concatenate([before, x, after], axis=dim)
    return x


def tv_local(padded):
    corner_cells = padded[:, :, :-1, :-1]
    down_diff = padded[:, :, 1:, :-1] - corner_cells
    right_diff = padded[:, :, :-1, 1:] - corner_cells
    weight = 1.0 / jnp.sqrt(
        jnp.sum(down_diff * down_diff + right_diff * right_diff, axis=1, keepdims=True) + tv_smooth
    )
    flow_down = weight * down_diff
    flow_right = weight * right_diff
    return (
        flow_down[:, :, :-1, 1:]
        + flow_right[:, :, 1:, :-1]
        - flow_down[:, :, 1:, 1:]
        - flow_right[:, :, 1:, 1:]
    )


def over_all(x):
    devices = lax.axis_size(BATCH_TILE)
    shares = lax.all_to_all(
        x.reshape(devices, -1, 128), BATCH_TILE, split_axis=0, concat_axis=0, tiled=True
    )
    mine = jnp.broadcast_to(jnp.sum(shares, 0, keepdims=True), shares.shape)
    return lax.all_to_all(mine, BATCH_TILE, split_axis=0, concat_axis=0, tiled=True).reshape(x.shape)


def on_device(object_field, probe_wave, intensities, owner_rows, offsets):
    local_rows = intensities.shape[0]
    nbatch = lax.axis_size(BATCH)
    slots_all = nbatch * CAP
    targets = owner_rows[:, 0]
    serial = jnp.arange(local_rows, dtype=jnp.int32)
    earlier = (targets[:, None] == targets[None, :]) & (serial[None, :] < serial[:, None])
    slot_of = targets * CAP + jnp.sum(earlier.astype(jnp.int32), axis=1)
    hit = slot_of[:, None] == jnp.arange(slots_all, dtype=jnp.int32)[None, :]
    request = jnp.sum(jnp.where(hit[:, :, None], offsets[:, None, :] + 1, 0), axis=0)
    wanted = lax.all_to_all(
        request.reshape(nbatch, CAP * 2), BATCH, split_axis=0, concat_axis=0, tiled=True
    ).reshape(slots_all * 2)
    sent = pack_call(slot_of, intensities)
    padded = extended(object_field, ((BATCH, 2),), 1)

    def exchange(one):
        return lax.all_to_all(one, BATCH, split_axis=0, concat_axis=0, tiled=True)

    ints_0 = exchange(sent[0])
    exits_0, psi_0 = forward_call(0, wanted, object_field, probe_wave)
    later, exits_0 = lax.optimization_barrier((sent[1], exits_0))
    ints_1 = exchange(later)
    exits_1, psi_1 = forward_call(1, wanted, object_field, probe_wave)
    half = backward_call(0, wanted, object_field, probe_wave, ints_0, exits_0, psi_0)
    field_grad, probe_local = backward_call(
        1, wanted, object_field, probe_wave, ints_1, exits_1, psi_1, *half
    )
    padded, probe_local = lax.optimization_barrier((padded, probe_local))
    probe_total = over_all(probe_local)
    padded = extended(padded, ((TILE, 3),), 1)
    new_object = object_field - update_rate * (field_grad + tv_weight * tv_local(padded))
    new_probe = probe_wave.astype(F32) - probe_rate * probe_total
    return (new_object, new_probe)


def solution(mesh):
    finer = Mesh(mesh.devices.reshape(4, 4, 4, 2), ("batch_0", "batch_1", "tile_0", "tile_1"))
    placed = (P(None, None, BATCH, TILE), P(), P(BATCH_TILE), P(BATCH_TILE), P(BATCH_TILE))
    return jax.shard_map(
        on_device,
        mesh=finer,
        in_specs=placed,
        out_specs=(P(None, None, BATCH, TILE), P()),
        check_vma=False,
    )
```

```python
import jax
import jax.numpy as jnp
import numpy as np
from jax import lax
from jax.experimental import pallas as pl
from jax.experimental.pallas import tpu as pltpu
from jax.sharding import Mesh
from jax.sharding import PartitionSpec as P

BATCH = ("batch_0", "batch_1")
TILE = ("tile_0", "tile_1")
BATCH_TILE = BATCH + TILE

update_rate = 0.1
tv_weight = 12.0
tv_smooth = 1.0
probe_rate = 0.04

N = 256
T = 384
CAP = 2
R = 32
PIECES = N // R
F32 = jnp.float32
BF16 = jnp.bfloat16


def tables():
    counter = np.arange(N)
    angles = (counter[:, None] * counter[None, :] % N) * (2.0 * np.pi / N)
    cos_table = (np.cos(angles) / np.sqrt(N)).astype(jnp.bfloat16)
    sin_table = (-np.sin(angles) / np.sqrt(N)).astype(jnp.bfloat16)
    freq = (counter + N // 2) % N - N // 2
    squared = (freq * freq).astype(np.float64)
    phases = -(0.5 / N) * (squared[:, None] + squared[None, :])
    prop = np.stack([np.cos(phases), np.sin(phases)]).astype(np.float32)
    return np.stack([cos_table, sin_table, -sin_table]), prop


def rows(j):
    return pl.ds(R * j, R)


def issue(acc, regs, pushes, lhs):
    for step in range(2):
        for q in range(2):
            pltpu.matmul_push_rhs(pushes[q][step], staging_register=regs[step], mxu_index=q)
        for j in range(PIECES):
            for q in range(2):
                pltpu.matmul_acc_lhs(
                    acc[q][j], lhs[q][step](j), load_staged_rhs=regs[step] if j == 0 else None
                )


def shared(start, acc, x, y, tab):
    row, col = start
    regs = (0, 1)
    lane = lax.broadcasted_iota(jnp.int32, (R, 128), 1)
    back = (128 - col) & 127
    forth = col & 127
    keep = lane < 128 - col
    moved = lane >= col

    def left(forward):
        sin, neg = (1, 2) if forward else (2, 1)
        xr, xi = x[0], x[1]
        issue(
            acc,
            regs,
            ((xr[...], xi[...]), (xr[...], xi[...])),
            (
                (lambda j: tab[0, rows(j)], lambda j: tab[neg, rows(j)]),
                (lambda j: tab[sin, rows(j)], lambda j: tab[0, rows(j)]),
            ),
        )

    def middle():
        for j in range(PIECES):
            for q in range(2):
                y[q][rows(j)] = pltpu.matmul_pop(acc[q][j]).astype(BF16)

    def right(forward):
        sin, neg = (1, 2) if forward else (2, 1)
        lhs = (lambda j: y[0][rows(j)], lambda j: y[1][rows(j)])
        issue(acc, regs, ((tab[0], tab[neg]), (tab[sin], tab[0])), (lhs, lhs))

    def pops(j):
        return pltpu.matmul_pop(acc[0][j]), pltpu.matmul_pop(acc[1][j])

    def cut(tile, s, q, j):
        at = pl.ds(row + R * j, R)
        turned = [pltpu.roll(tile[s, q, k, at, :], back, 1) for k in range(3)]
        return jnp.concatenate(
            [jnp.where(keep, turned[0], turned[1]), jnp.where(keep, turned[1], turned[2])], 1
        )

    def put(field, s, q, j, value):
        value = value.astype(BF16).astype(F32)
        turned = [pltpu.roll(value[:, 128 * k : 128 * k + 128], forth, 1) for k in range(2)]
        parts = (
            jnp.where(moved, turned[0], 0.0),
            jnp.where(moved, turned[1], turned[0]),
            jnp.where(moved, 0.0, turned[1]),
        )
        at = pl.ds(row + R * j, R)
        for k in range(3):
            field[s, q, k, at, :] = field[s, q, k, at, :] + parts[k]

    def kick(prop, sign):
        for j in range(PIECES):
            fr, fi = pops(j)
            hr, hi = prop[0, rows(j)], prop[1, rows(j)]
            if sign > 0:
                x[0][rows(j)] = (hr * fr - hi * fi).astype(BF16)
                x[1][rows(j)] = (hr * fi + hi * fr).astype(BF16)
            else:
                x[0][rows(j)] = (hr * fr + hi * fi).astype(BF16)
                x[1][rows(j)] = (hr * fi - hi * fr).astype(BF16)

    return left, middle, right, pops, cut, put, kick


def forward_steps(env, start, acc, x, y, psi, exits):
    tile, probe, tab, prop = env
    left, middle, right, pops, cut, _, kick = shared(start, acc, x, y, tab)
    for j in range(PIECES):
        tr, ti = cut(tile, 0, 0, j), cut(tile, 0, 1, j)
        pr, pi = probe[0, rows(j)].astype(F32), probe[1, rows(j)].astype(F32)
        x[0][rows(j)] = (pr * tr - pi * ti).astype(BF16)
        x[1][rows(j)] = (pr * ti + pi * tr).astype(BF16)
    left(True)
    yield
    middle()
    right(True)
    yield
    kick(prop, 1)
    left(False)
    yield
    middle()
    right(False)
    yield
    for j in range(PIECES):
        wr, wi = pops(j)
        wr, wi = wr.astype(BF16), wi.astype(BF16)
        psi[0, rows(j)] = wr
        psi[1, rows(j)] = wi
        wr, wi = wr.astype(F32), wi.astype(F32)
        tr, ti = cut(tile, 1, 0, j), cut(tile, 1, 1, j)
        x[0][rows(j)] = (wr * tr - wi * ti).astype(BF16)
        x[1][rows(j)] = (wr * ti + wi * tr).astype(BF16)
    left(True)
    yield
    middle()
    right(True)
    yield
    for j in range(PIECES):
        er, ei = pops(j)
        exits[0, rows(j)] = er
        exits[1, rows(j)] = ei


def backward_steps(env, start, scale, ints, acc, x, y, psi, exits, field):
    tile, probe, tab, prop, probe_sum = env
    left, middle, right, pops, cut, put, kick = shared(start, acc, x, y, tab)
    for j in range(PIECES):
        er, ei = exits[0, rows(j)], exits[1, rows(j)]
        misfit = scale * (er * er + ei * ei - ints[rows(j)].astype(F32))
        x[0][rows(j)] = (misfit * er).astype(BF16)
        x[1][rows(j)] = (misfit * ei).astype(BF16)
    left(False)
    yield
    middle()
    right(False)
    yield
    for j in range(PIECES):
        gr, gi = pops(j)
        wr, wi = psi[0, rows(j)].astype(F32), psi[1, rows(j)].astype(F32)
        tr, ti = cut(tile, 1, 0, j), cut(tile, 1, 1, j)
        x[0][rows(j)] = (gr * tr + gi * ti).astype(BF16)
        x[1][rows(j)] = (gi * tr - gr * ti).astype(BF16)
        put(field, 1, 0, j, gr * wr + gi * wi)
        put(field, 1, 1, j, gi * wr - gr * wi)
    left(False)
    yield
    middle()
    right(False)
    yield
    kick(prop, -1)
    left(True)
    yield
    middle()
    right(True)
    yield
    for j in range(PIECES):
        gr, gi = pops(j)
        wr, wi = probe[0, rows(j)].astype(F32), probe[1, rows(j)].astype(F32)
        tr, ti = cut(tile, 0, 0, j), cut(tile, 0, 1, j)
        probe_sum[0, rows(j)] = probe_sum[0, rows(j)] + (gr * tr + gi * ti)
        probe_sum[1, rows(j)] = probe_sum[1, rows(j)] + (gi * tr - gr * ti)
        put(field, 0, 0, j, gr * wr + gi * wi)
        put(field, 0, 1, j, gi * wr - gr * wi)


def interleave(*steps):
    live = list(steps)
    while live:
        for one in list(live):
            if next(one, 1) == 1:
                live.remove(one)


def list_used(wanted, listed):
    def one(k, used):
        listed[used] = k
        return used + (wanted[2 * k] > 0).astype(jnp.int32)

    return lax.fori_loop(0, SLOTS, one, jnp.int32(0))


def chosen(wanted, listed, count, pair):
    there = 2 * pair + 1 < count
    slots = listed[2 * pair], listed[jnp.where(there, 2 * pair + 1, 2 * pair)]
    return slots, [(wanted[2 * k] - 1, wanted[2 * k + 1] - 1) for k in slots], there


def round_tile(tile_in, tile):
    for s in range(2):
        for q in range(2):
            for k in range(3):
                tile[s, q, k] = tile_in[s, q, :, pl.ds(128 * k, 128)].astype(BF16).astype(F32)


def with_accumulators(body):
    def start(acc_a, acc_b):
        for one in acc_a + acc_b:
            for ref in one:
                pltpu.matmul_pop(ref)
        body(acc_a, acc_b)

    refs = tuple(tuple(pltpu.ACC(q)((R, N), F32) for _ in range(PIECES)) for q in range(2))
    pl.run_scoped(start, refs, refs)


def forward_kernel(
    wanted, tile_in, probe, tab, prop, exits_out, psi_out, edge_rows, edge_cols, tile, listed, x, y, exits, psi, sems
):
    round_tile(tile_in, tile)
    for s in range(2):
        for q in range(2):
            k = 2 * s + q
            edge_rows[k : k + 1] = tile_in[s, q, 0:1, :]
            edge_rows[4 + k : 5 + k] = tile_in[s, q, T - 1 : T, :]
            edge_cols[k : k + 1] = jnp.transpose(tile_in[s, q, :, 0:128])[0:1]
            edge_cols[4 + k : 5 + k] = jnp.transpose(tile_in[s, q, :, T - 128 : T])[127:128]
    env = (tile, probe, tab, prop)
    count = list_used(wanted, listed)
    pairs = (count + 1) // 2

    def copies(b, at):
        return (
            pltpu.make_async_copy(exits.at[b], exits_out.at[at], sems.at[0, b]),
            pltpu.make_async_copy(psi.at[b], psi_out.at[at], sems.at[1, b]),
        )

    def body(acc_a, acc_b):
        @pl.loop(0, pairs)
        def _(pair):
            b = pair % 2
            _, at, _ = chosen(wanted, listed, count, pair)

            @pl.when(pair >= 2)
            def _():
                for one in copies(b, pair - 2):
                    one.wait()

            interleave(
                *[
                    forward_steps(
                        env,
                        at[i],
                        (acc_a, acc_b)[i],
                        (x.at[i, 0], x.at[i, 1]),
                        (y.at[i, 0], y.at[i, 1]),
                        psi.at[b, i],
                        exits.at[b, i],
                    )
                    for i in range(2)
                ]
            )
            for one in copies(b, pair):
                one.start()

        for late in (2, 1):

            @pl.when(pairs >= late)
            def _():
                for one in copies((pairs - late) % 2, pairs - late):
                    one.wait()

    with_accumulators(body)


def backward_kernel(
    wanted, tile_in, probe, tab, prop, ints, exits_in, psi_in, field_out, probe_sum, *scratch
):
    tile, field_a, field_b, listed, x, y, exits, psi, sems = scratch
    count = list_used(wanted, listed)
    pairs = (count + 1) // 2

    def copies(b, at):
        return (
            pltpu.make_async_copy(exits_in.at[at], exits.at[b], sems.at[0, b]),
            pltpu.make_async_copy(psi_in.at[at], psi.at[b], sems.at[1, b]),
        )

    @pl.when(pairs > 0)
    def _():
        for one in copies(0, 0):
            one.start()

    round_tile(tile_in, tile)
    for field in (field_a, field_b):
        for s in range(2):
            for q in range(2):
                for k in range(3):
                    field[s, q, k] = jnp.zeros((T, 128), F32)
    probe_sum[...] = jnp.zeros((2, N, N), F32)
    env = (tile, probe, tab, prop, probe_sum)

    def body(acc_a, acc_b):
        @pl.loop(0, pairs)
        def _(pair):
            b = pair % 2
            slots, at, there = chosen(wanted, listed, count, pair)

            @pl.when(pair + 1 < pairs)
            def _():
                for one in copies(1 - b, pair + 1):
                    one.start()

            for one in copies(b, pair):
                one.wait()
            scales = F32(0.5), jnp.where(there, F32(0.5), F32(0.0))
            interleave(
                *[
                    backward_steps(
                        env,
                        at[i],
                        scales[i],
                        ints.at[slots[i]],
                        (acc_a, acc_b)[i],
                        (x.at[i, 0], x.at[i, 1]),
                        (y.at[i, 0], y.at[i, 1]),
                        psi.at[b, i],
                        exits.at[b, i],
                        (field_a, field_b)[i],
                    )
                    for i in range(2)
                ]
            )

    with_accumulators(body)
    for s in range(2):
        for q in range(2):
            for k in range(3):
                field_out[s, q, :, pl.ds(128 * k, 128)] = field_a[s, q, k] + field_b[s, q, k]


def finish_kernel(tile, field, edge_rows, edge_cols, out, padded, flat):
    flat[...] = jnp.zeros((128, 512), F32)
    flat[0:8] = edge_cols[...]
    tall = jnp.transpose(flat[...])
    for s in range(2):
        for q in range(2):
            k = 2 * s + q
            padded[s, q, 8 : 8 + T, 128 : 128 + T] = tile[s, q]
            padded[s, q, 7:8, 128 : 128 + T] = edge_rows[k : k + 1]
            padded[s, q, 8 + T : 9 + T, 128 : 128 + T] = edge_rows[4 + k : 5 + k]
            after, before = tall[:, k : k + 1], tall[:, 4 + k : 5 + k]
            padded[s, q, 8 : 8 + T, 128 + T : 256 + T] = jnp.broadcast_to(after[:T], (T, 128))
            padded[s, q, 8 : 8 + T, 0:128] = jnp.broadcast_to(before[:T], (T, 128))
            padded[s, q, 7:8, 128 + T : 256 + T] = jnp.broadcast_to(after[T : T + 1], (1, 128))
            padded[s, q, 8 + T : 9 + T, 0:128] = jnp.broadcast_to(before[T : T + 1], (1, 128))
    for s in range(2):

        def part(at, down, right):
            here = [padded[s, q, at + 8 + down : at + 8 + down + 16, 128 + right : 128 + right + T] for q in range(2)]
            return here

        for at in range(0, T, 16):
            here, below, right = part(at, 0, 0), part(at, 1, 0), part(at, 0, 1)
            above, above_right = part(at, -1, 0), part(at, -1, 1)
            left, left_below = part(at, 0, -1), part(at, 1, -1)

            def slopes(one, lower, righter):
                dy = [b - a for a, b in zip(one, lower)]
                dx = [b - a for a, b in zip(one, righter)]
                total = dy[0] * dy[0] + dx[0] * dx[0] + (dy[1] * dy[1] + dx[1] * dx[1])
                return dy, dx, 1.0 / jnp.sqrt(total + tv_smooth)

            dy, dx, m = slopes(here, below, right)
            dy_up, _, m_up = slopes(above, here, above_right)
            _, dx_left, m_left = slopes(left, left_below, here)
            for q in range(2):
                tv = m_up * dy_up[q] + m_left * dx_left[q] - m * dy[q] - m * dx[q]
                grad = field[s, q, at : at + 16] + tv_weight * tv
                out[s, q, at : at + 16] = here[q] - update_rate * grad


VMEM = pl.BlockSpec(memory_space=pltpu.VMEM)
SMEM = pl.BlockSpec(memory_space=pltpu.SMEM)
HBM = pl.BlockSpec(memory_space=pltpu.HBM)
SOURCES = 16
SLOTS = SOURCES * CAP
PAIRS = SLOTS // 2
WIDE = pltpu.VMEM((2, 2, 3, T, 128), F32)
TWO = pltpu.VMEM((2, 2, N, N), BF16)
FRONTS = [
    pltpu.VMEM((2, 2, 2, N, N), F32),
    pltpu.VMEM((2, 2, 2, N, N), BF16),
    pltpu.SemaphoreType.DMA((2, 2)),
]
LISTED = pltpu.SMEM((SLOTS + 1,), jnp.int32)


def params(limit):
    flops = SLOTS * 3 * 2 * 8 * N**3
    return dict(
        compiler_params=pltpu.CompilerParams(vmem_limit_bytes=limit << 20),
        cost_estimate=pl.CostEstimate(flops=flops, transcendentals=0, bytes_accessed=32 << 20),
    )


def forward_call(wanted, tile, probe):
    tab, prop = tables()
    return pl.pallas_call(
        forward_kernel,
        out_shape=(
            jax.ShapeDtypeStruct((PAIRS, 2, 2, N, N), F32),
            jax.ShapeDtypeStruct((PAIRS, 2, 2, N, N), BF16),
            jax.ShapeDtypeStruct((8, T), F32),
            jax.ShapeDtypeStruct((8, T), F32),
        ),
        in_specs=[SMEM] + [VMEM] * 4,
        out_specs=(HBM, HBM, VMEM, VMEM),
        scratch_shapes=[WIDE, LISTED, TWO, TWO] + FRONTS,
        name="forward",
        **params(57),
    )(wanted, tile, probe, tab, prop)


def backward_call(wanted, tile, probe, ints, exits, psi):
    tab, prop = tables()
    return pl.pallas_call(
        backward_kernel,
        out_shape=(jax.ShapeDtypeStruct((2, 2, T, T), F32), jax.ShapeDtypeStruct((2, N, N), F32)),
        in_specs=[SMEM] + [VMEM] * 5 + [HBM, HBM],
        out_specs=(VMEM, VMEM),
        scratch_shapes=[WIDE, WIDE, WIDE, LISTED, TWO, TWO] + FRONTS,
        name="backward",
        **params(57),
    )(wanted, tile, probe, tab, prop, ints, exits, psi)


def finish_call(tile, field, edge_rows, edge_cols):
    return pl.pallas_call(
        finish_kernel,
        out_shape=jax.ShapeDtypeStruct((2, 2, T, T), F32),
        in_specs=[VMEM] * 4,
        out_specs=VMEM,
        scratch_shapes=[pltpu.VMEM((2, 2, T + 16, T + 256), F32), pltpu.VMEM((128, 512), F32)],
        compiler_params=pltpu.CompilerParams(vmem_limit_bytes=24 << 20),
        name="finish",
    )(tile, field, edge_rows, edge_cols)


def pack_kernel(slots, values, out):
    for i in range(SOURCES):
        out[slots[i]] = values[i].astype(BF16)


def pack_call(slots, intensities):
    return pl.pallas_call(
        pack_kernel,
        out_shape=jax.ShapeDtypeStruct((SLOTS, N, N), BF16),
        in_specs=[SMEM, VMEM],
        out_specs=VMEM,
        compiler_params=pltpu.CompilerParams(vmem_limit_bytes=24 << 20),
        name="pack",
    )(slots, intensities)


def moved(x, axis, step):
    size = lax.axis_size(axis)
    return lax.ppermute(x, axis, [(i, (i + step) % size) for i in range(size)])


def neighbours(edge_rows, edge_cols):
    above, below = moved(edge_rows[4:], BATCH, 1), moved(edge_rows[:4], BATCH, -1)
    for_left = jnp.concatenate([edge_cols[:4], jnp.broadcast_to(above[:, :1], (4, 128))], 1)
    for_right = jnp.concatenate([edge_cols[4:], jnp.broadcast_to(below[:, -1:], (4, 128))], 1)
    right, left = moved(for_left, TILE, -1), moved(for_right, TILE, 1)
    return jnp.concatenate([above, below]), jnp.concatenate([right, left])


def over_all(x):
    devices = lax.axis_size(BATCH_TILE)
    shares = lax.all_to_all(
        x.astype(BF16).reshape(devices, -1, 128), BATCH_TILE, split_axis=0, concat_axis=0, tiled=True
    )
    mine = jnp.sum(shares.astype(F32), 0, keepdims=True).astype(BF16)
    mine = jnp.broadcast_to(mine, shares.shape)
    total = lax.all_to_all(mine, BATCH_TILE, split_axis=0, concat_axis=0, tiled=True)
    return total.astype(F32).reshape(x.shape)


def on_device(object_field, probe_wave, intensities, owner_rows, offsets):
    local_rows = intensities.shape[0]
    nbatch = lax.axis_size(BATCH)
    slots_all = nbatch * CAP
    targets = owner_rows[:, 0]
    serial = jnp.arange(local_rows, dtype=jnp.int32)
    earlier = (targets[:, None] == targets[None, :]) & (serial[None, :] < serial[:, None])
    slot_of = targets * CAP + jnp.sum(earlier.astype(jnp.int32), axis=1)
    hit = slot_of[:, None] == jnp.arange(slots_all, dtype=jnp.int32)[None, :]
    request = jnp.sum(jnp.where(hit[:, :, None], offsets[:, None, :] + 1, 0), axis=0)
    wanted = lax.all_to_all(
        request.reshape(nbatch, CAP * 2), BATCH, split_axis=0, concat_axis=0, tiled=True
    ).reshape(slots_all * 2)
    sent = pack_call(slot_of, intensities).reshape(nbatch, CAP, N, N)
    ints = lax.all_to_all(sent, BATCH, split_axis=0, concat_axis=0, tiled=True)
    ints = ints.reshape(slots_all, N, N)
    exits, psi, edge_rows, edge_cols = forward_call(wanted, object_field, probe_wave)
    around = neighbours(edge_rows, edge_cols)
    field_grad, probe_local = backward_call(wanted, object_field, probe_wave, ints, exits, psi)
    probe_total = over_all(probe_local)
    new_object = finish_call(object_field, field_grad, *around)
    new_probe = probe_wave.astype(F32) - probe_rate * probe_total
    return (new_object, new_probe)


def solution(mesh):
    finer = Mesh(mesh.devices.reshape(4, 4, 4, 2), ("batch_0", "batch_1", "tile_0", "tile_1"))
    placed = (P(None, None, BATCH, TILE), P(), P(BATCH_TILE), P(BATCH_TILE), P(BATCH_TILE))
    return jax.shard_map(
        on_device,
        mesh=finer,
        in_specs=placed,
        out_specs=(P(None, None, BATCH, TILE), P()),
        check_vma=False,
    )
```

```python
import jax
import jax.numpy as jnp
import numpy as np
from jax import lax
from jax.experimental import pallas as pl
from jax.experimental.pallas import tpu as pltpu
from jax.sharding import Mesh
from jax.sharding import PartitionSpec as P

BATCH = ("batch_0", "batch_1")
TILE = ("tile_0", "tile_1")
BATCH_TILE = BATCH + TILE

update_rate = 0.1
tv_weight = 12.0
tv_smooth = 1.0
probe_rate = 0.04

N = 256
T = 384
CAP = 2
R = 32
PIECES = N // R
F32 = jnp.float32
BF16 = jnp.bfloat16


def tables():
    counter = np.arange(N)
    angles = (counter[:, None] * counter[None, :] % N) * (2.0 * np.pi / N)
    cos_table = (np.cos(angles) / np.sqrt(N)).astype(jnp.bfloat16)
    sin_table = (-np.sin(angles) / np.sqrt(N)).astype(jnp.bfloat16)
    freq = (counter + N // 2) % N - N // 2
    squared = (freq * freq).astype(np.float64)
    phases = -(0.5 / N) * (squared[:, None] + squared[None, :])
    prop = np.stack([np.cos(phases), np.sin(phases)]).astype(np.float32)
    return np.stack([cos_table, sin_table, -sin_table]), prop


def rows(j):
    return pl.ds(R * j, R)


def issue(acc, regs, pushes, lhs):
    for step in range(2):
        for q in range(2):
            pltpu.matmul_push_rhs(pushes[q][step], staging_register=regs[step], mxu_index=q)
        for j in range(PIECES):
            for q in range(2):
                pltpu.matmul_acc_lhs(
                    acc[q][j], lhs[q][step](j), load_staged_rhs=regs[step] if j == 0 else None
                )


def shared(start, acc, x, y, tab):
    row, col = start
    regs = (0, 1)
    lane = lax.broadcasted_iota(jnp.int32, (R, 128), 1)
    back = (128 - col) & 127
    forth = col & 127
    keep = lane < 128 - col
    moved = lane >= col

    def left(forward):
        sin, neg = (1, 2) if forward else (2, 1)
        xr, xi = x[0], x[1]
        issue(
            acc,
            regs,
            ((xr[...], xi[...]), (xr[...], xi[...])),
            (
                (lambda j: tab[0, rows(j)], lambda j: tab[neg, rows(j)]),
                (lambda j: tab[sin, rows(j)], lambda j: tab[0, rows(j)]),
            ),
        )

    def middle():
        for j in range(PIECES):
            for q in range(2):
                y[q][rows(j)] = pltpu.matmul_pop(acc[q][j]).astype(BF16)

    def right(forward):
        sin, neg = (1, 2) if forward else (2, 1)
        lhs = (lambda j: y[0][rows(j)], lambda j: y[1][rows(j)])
        issue(acc, regs, ((tab[0], tab[neg]), (tab[sin], tab[0])), (lhs, lhs))

    def pops(j):
        return pltpu.matmul_pop(acc[0][j]), pltpu.matmul_pop(acc[1][j])

    def cut(tile, s, q, j):
        at = pl.ds(row + R * j, R)
        turned = [pltpu.roll(tile[s, q, k, at, :], back, 1) for k in range(3)]
        return jnp.concatenate(
            [jnp.where(keep, turned[0], turned[1]), jnp.where(keep, turned[1], turned[2])], 1
        )

    def put(field, s, q, j, value):
        value = value.astype(BF16).astype(F32)
        turned = [pltpu.roll(value[:, 128 * k : 128 * k + 128], forth, 1) for k in range(2)]
        parts = (
            jnp.where(moved, turned[0], 0.0),
            jnp.where(moved, turned[1], turned[0]),
            jnp.where(moved, 0.0, turned[1]),
        )
        at = pl.ds(row + R * j, R)
        for k in range(3):
            field[s, q, k, at, :] = field[s, q, k, at, :] + parts[k]

    def kick(prop, sign):
        for j in range(PIECES):
            fr, fi = pops(j)
            hr, hi = prop[0, rows(j)], prop[1, rows(j)]
            if sign > 0:
                x[0][rows(j)] = (hr * fr - hi * fi).astype(BF16)
                x[1][rows(j)] = (hr * fi + hi * fr).astype(BF16)
            else:
                x[0][rows(j)] = (hr * fr + hi * fi).astype(BF16)
                x[1][rows(j)] = (hr * fi - hi * fr).astype(BF16)

    return left, middle, right, pops, cut, put, kick


def forward_steps(env, start, acc, x, y, psi, exits):
    tile, probe, tab, prop = env
    left, middle, right, pops, cut, _, kick = shared(start, acc, x, y, tab)
    for j in range(PIECES):
        tr, ti = cut(tile, 0, 0, j), cut(tile, 0, 1, j)
        pr, pi = probe[0, rows(j)].astype(F32), probe[1, rows(j)].astype(F32)
        x[0][rows(j)] = (pr * tr - pi * ti).astype(BF16)
        x[1][rows(j)] = (pr * ti + pi * tr).astype(BF16)
    left(True)
    yield
    middle()
    right(True)
    yield
    kick(prop, 1)
    left(False)
    yield
    middle()
    right(False)
    yield
    for j in range(PIECES):
        wr, wi = pops(j)
        wr, wi = wr.astype(BF16), wi.astype(BF16)
        psi[0, rows(j)] = wr
        psi[1, rows(j)] = wi
        wr, wi = wr.astype(F32), wi.astype(F32)
        tr, ti = cut(tile, 1, 0, j), cut(tile, 1, 1, j)
        x[0][rows(j)] = (wr * tr - wi * ti).astype(BF16)
        x[1][rows(j)] = (wr * ti + wi * tr).astype(BF16)
    left(True)
    yield
    middle()
    right(True)
    yield
    for j in range(PIECES):
        er, ei = pops(j)
        exits[0, rows(j)] = er
        exits[1, rows(j)] = ei


def backward_steps(env, start, scale, ints, acc, x, y, psi, exits, field):
    tile, probe, tab, prop, probe_sum = env
    left, middle, right, pops, cut, put, kick = shared(start, acc, x, y, tab)
    for j in range(PIECES):
        er, ei = exits[0, rows(j)], exits[1, rows(j)]
        misfit = scale * (er * er + ei * ei - ints[rows(j)].astype(F32))
        x[0][rows(j)] = (misfit * er).astype(BF16)
        x[1][rows(j)] = (misfit * ei).astype(BF16)
    left(False)
    yield
    middle()
    right(False)
    yield
    for j in range(PIECES):
        gr, gi = pops(j)
        wr, wi = psi[0, rows(j)].astype(F32), psi[1, rows(j)].astype(F32)
        tr, ti = cut(tile, 1, 0, j), cut(tile, 1, 1, j)
        x[0][rows(j)] = (gr * tr + gi * ti).astype(BF16)
        x[1][rows(j)] = (gi * tr - gr * ti).astype(BF16)
        put(field, 1, 0, j, gr * wr + gi * wi)
        put(field, 1, 1, j, gi * wr - gr * wi)
    left(False)
    yield
    middle()
    right(False)
    yield
    kick(prop, -1)
    left(True)
    yield
    middle()
    right(True)
    yield
    for j in range(PIECES):
        gr, gi = pops(j)
        wr, wi = probe[0, rows(j)].astype(F32), probe[1, rows(j)].astype(F32)
        tr, ti = cut(tile, 0, 0, j), cut(tile, 0, 1, j)
        probe_sum[0, rows(j)] = probe_sum[0, rows(j)] + (gr * tr + gi * ti)
        probe_sum[1, rows(j)] = probe_sum[1, rows(j)] + (gi * tr - gr * ti)
        put(field, 0, 0, j, gr * wr + gi * wi)
        put(field, 0, 1, j, gi * wr - gr * wi)


def interleave(*steps):
    live = list(steps)
    while live:
        for one in list(live):
            if next(one, 1) == 1:
                live.remove(one)


def list_used(wanted, listed):
    def one(k, used):
        listed[used] = k
        return used + (wanted[2 * k] > 0).astype(jnp.int32)

    return lax.fori_loop(0, SLOTS, one, jnp.int32(0))


def chosen(wanted, listed, count, pair):
    there = 2 * pair + 1 < count
    slots = listed[2 * pair], listed[jnp.where(there, 2 * pair + 1, 2 * pair)]
    return slots, [(wanted[2 * k] - 1, wanted[2 * k + 1] - 1) for k in slots], there


def round_tile(tile_in, tile):
    for s in range(2):
        for q in range(2):
            for k in range(3):
                tile[s, q, k] = tile_in[s, q, :, pl.ds(128 * k, 128)].astype(BF16).astype(F32)


def with_accumulators(body):
    def start(acc_a, acc_b):
        for one in acc_a + acc_b:
            for ref in one:
                pltpu.matmul_pop(ref)
        body(acc_a, acc_b)

    refs = tuple(tuple(pltpu.ACC(q)((R, N), F32) for _ in range(PIECES)) for q in range(2))
    pl.run_scoped(start, refs, refs)


def forward_kernel(
    wanted, tile_in, probe, tab, prop, exits_out, psi_out, edge_rows, edge_cols, tile, listed, x, y, exits, psi, sems
):
    round_tile(tile_in, tile)
    for s in range(2):
        for q in range(2):
            k = 2 * s + q
            edge_rows[k : k + 1] = tile_in[s, q, 0:1, :]
            edge_rows[4 + k : 5 + k] = tile_in[s, q, T - 1 : T, :]
            edge_cols[k : k + 1] = jnp.transpose(tile_in[s, q, :, 0:128])[0:1]
            edge_cols[4 + k : 5 + k] = jnp.transpose(tile_in[s, q, :, T - 128 : T])[127:128]
    env = (tile, probe, tab, prop)
    count = list_used(wanted, listed)
    pairs = (count + 1) // 2

    def copies(b, at):
        return (
            pltpu.make_async_copy(exits.at[b], exits_out.at[at], sems.at[0, b]),
            pltpu.make_async_copy(psi.at[b], psi_out.at[at], sems.at[1, b]),
        )

    def body(acc_a, acc_b):
        @pl.loop(0, pairs)
        def _(pair):
            b = pair % 2
            _, at, _ = chosen(wanted, listed, count, pair)

            @pl.when(pair >= 2)
            def _():
                for one in copies(b, pair - 2):
                    one.wait()

            interleave(
                *[
                    forward_steps(
                        env,
                        at[i],
                        (acc_a, acc_b)[i],
                        (x.at[i, 0], x.at[i, 1]),
                        (y.at[i, 0], y.at[i, 1]),
                        psi.at[b, i],
                        exits.at[b, i],
                    )
                    for i in range(2)
                ]
            )
            for one in copies(b, pair):
                one.start()

        for late in (2, 1):

            @pl.when(pairs >= late)
            def _():
                for one in copies((pairs - late) % 2, pairs - late):
                    one.wait()

    with_accumulators(body)


def backward_kernel(
    wanted, tile_in, probe, tab, prop, ints, exits_in, psi_in, field_out, probe_out, *scratch
):
    tile, field_a, field_b, probe_sum, listed, x, y, exits, psi, sems = scratch
    count = list_used(wanted, listed)
    pairs = (count + 1) // 2

    def copies(b, at):
        return (
            pltpu.make_async_copy(exits_in.at[at], exits.at[b], sems.at[0, b]),
            pltpu.make_async_copy(psi_in.at[at], psi.at[b], sems.at[1, b]),
        )

    @pl.when(pairs > 0)
    def _():
        for one in copies(0, 0):
            one.start()

    round_tile(tile_in, tile)
    for field in (field_a, field_b):
        for s in range(2):
            for q in range(2):
                for k in range(3):
                    field[s, q, k] = jnp.zeros((T, 128), F32)
    probe_sum[...] = jnp.zeros((2, N, N), F32)
    env = (tile, probe, tab, prop, probe_sum)

    def body(acc_a, acc_b):
        @pl.loop(0, pairs)
        def _(pair):
            b = pair % 2
            slots, at, there = chosen(wanted, listed, count, pair)

            @pl.when(pair + 1 < pairs)
            def _():
                for one in copies(1 - b, pair + 1):
                    one.start()

            for one in copies(b, pair):
                one.wait()
            scales = F32(0.5), jnp.where(there, F32(0.5), F32(0.0))
            interleave(
                *[
                    backward_steps(
                        env,
                        at[i],
                        scales[i],
                        ints.at[slots[i]],
                        (acc_a, acc_b)[i],
                        (x.at[i, 0], x.at[i, 1]),
                        (y.at[i, 0], y.at[i, 1]),
                        psi.at[b, i],
                        exits.at[b, i],
                        (field_a, field_b)[i],
                    )
                    for i in range(2)
                ]
            )

    with_accumulators(body)
    for s in range(2):
        for q in range(2):
            for k in range(3):
                field_out[s, q, :, pl.ds(128 * k, 128)] = field_a[s, q, k] + field_b[s, q, k]
    for q in range(2):
        for c in range(2):
            for j in range(N // 8):
                share = probe_sum[q, 8 * j : 8 * j + 8, 128 * c : 128 * c + 128]
                probe_out[SHARES // 2 * q + N // 8 * c + j] = share.astype(BF16)


def finish_kernel(tile, field, edge_rows, edge_cols, out, padded, flow_y, flow_x, flat):
    flat[...] = jnp.zeros((128, 512), F32)
    flat[0:8] = edge_cols[...]
    tall = jnp.transpose(flat[...])
    for s in range(2):
        for q in range(2):
            k = 2 * s + q
            for block, side in ((0, 4 + k), (4, k)):
                values = jnp.broadcast_to(tall[: T + 8, side : side + 1], (T + 8, 128))
                padded[s, q, block, 8 : 8 + T] = values[:T]
                padded[s, q, block, 0:8] = values[T:]
                padded[s, q, block, 8 + T : 16 + T] = values[T:]
            for c in range(3):
                at = slice(128 * c, 128 * c + 128)
                padded[s, q, 1 + c, 8 : 8 + T] = tile[s, q, :, at]
                padded[s, q, 1 + c, 0:8] = jnp.broadcast_to(edge_rows[k : k + 1, at], (8, 128))
                padded[s, q, 1 + c, 8 + T : 16 + T] = jnp.broadcast_to(
                    edge_rows[4 + k : 5 + k, at], (8, 128)
                )
    high = 56
    lane = lax.broadcasted_iota(jnp.int32, (high, 128), 1)
    for s in range(2):
        for at in range(0, T + 8, high):
            for c in range(4):
                dy, dx = [], []
                for q in range(2):
                    here = padded[s, q, c, at : at + high]
                    after = padded[s, q, c + 1, at : at + high]
                    dy.append(padded[s, q, c, at + 1 : at + 1 + high] - here)
                    right = jnp.where(lane == 127, pltpu.roll(after, 127, 1), pltpu.roll(here, 127, 1))
                    dx.append(right - here)
                total = dy[0] * dy[0] + dx[0] * dx[0] + (dy[1] * dy[1] + dx[1] * dx[1])
                m = lax.rsqrt(total + tv_smooth)
                for q in range(2):
                    flow_y[s, q, c, at : at + high] = m * dy[q]
                    flow_x[s, q, c, at : at + high] = m * dx[q]
    high = 64
    lane = lax.broadcasted_iota(jnp.int32, (high, 128), 1)
    for s in range(2):
        for q in range(2):
            for at in range(0, T, high):
                for c in range(1, 4):
                    low = at + 8
                    down = flow_y[s, q, c, low : low + high]
                    above = flow_y[s, q, c, low - 1 : low - 1 + high]
                    right = flow_x[s, q, c, low : low + high]
                    before = flow_x[s, q, c - 1, low : low + high]
                    left = jnp.where(lane == 0, pltpu.roll(before, 1, 1), pltpu.roll(right, 1, 1))
                    to = slice(128 * c - 128, 128 * c)
                    grad = field[s, q, at : at + high, to] + tv_weight * (above + left - down - right)
                    out[s, q, at : at + high, to] = padded[s, q, c, low : low + high] - update_rate * grad


VMEM = pl.BlockSpec(memory_space=pltpu.VMEM)
SMEM = pl.BlockSpec(memory_space=pltpu.SMEM)
HBM = pl.BlockSpec(memory_space=pltpu.HBM)
SOURCES = 16
SLOTS = SOURCES * CAP
PAIRS = SLOTS // 2
SHARES = 2 * N * N // (8 * 128)
WIDE = pltpu.VMEM((2, 2, 3, T, 128), F32)
TWO = pltpu.VMEM((2, 2, N, N), BF16)
FRONTS = [
    pltpu.VMEM((2, 2, 2, N, N), F32),
    pltpu.VMEM((2, 2, 2, N, N), BF16),
    pltpu.SemaphoreType.DMA((2, 2)),
]
LISTED = pltpu.SMEM((SLOTS + 1,), jnp.int32)


def params(limit):
    flops = SLOTS * 3 * 2 * 8 * N**3
    return dict(
        compiler_params=pltpu.CompilerParams(vmem_limit_bytes=limit << 20),
        cost_estimate=pl.CostEstimate(flops=flops, transcendentals=0, bytes_accessed=32 << 20),
    )


def forward_call(wanted, tile, probe):
    tab, prop = tables()
    return pl.pallas_call(
        forward_kernel,
        out_shape=(
            jax.ShapeDtypeStruct((PAIRS, 2, 2, N, N), F32),
            jax.ShapeDtypeStruct((PAIRS, 2, 2, N, N), BF16),
            jax.ShapeDtypeStruct((8, T), F32),
            jax.ShapeDtypeStruct((8, T), F32),
        ),
        in_specs=[SMEM] + [VMEM] * 4,
        out_specs=(HBM, HBM, VMEM, VMEM),
        scratch_shapes=[WIDE, LISTED, TWO, TWO] + FRONTS,
        name="forward",
        **params(57),
    )(wanted, tile, probe, tab, prop)


def backward_call(wanted, tile, probe, ints, exits, psi):
    tab, prop = tables()
    return pl.pallas_call(
        backward_kernel,
        out_shape=(jax.ShapeDtypeStruct((2, 2, T, T), F32), jax.ShapeDtypeStruct((SHARES, 8, 128), BF16)),
        in_specs=[SMEM] + [VMEM] * 5 + [HBM, HBM],
        out_specs=(VMEM, VMEM),
        scratch_shapes=[WIDE, WIDE, WIDE, pltpu.VMEM((2, N, N), F32), LISTED, TWO, TWO] + FRONTS,
        name="backward",
        **params(57),
    )(wanted, tile, probe, tab, prop, ints, exits, psi)


def finish_call(tile, field, edge_rows, edge_cols):
    return pl.pallas_call(
        finish_kernel,
        out_shape=jax.ShapeDtypeStruct((2, 2, T, T), F32),
        in_specs=[VMEM] * 4,
        out_specs=VMEM,
        scratch_shapes=[
            pltpu.VMEM((2, 2, 5, T + 16, 128), F32),
            pltpu.VMEM((2, 2, 4, T + 8, 128), F32),
            pltpu.VMEM((2, 2, 4, T + 8, 128), F32),
            pltpu.VMEM((128, 512), F32),
        ],
        compiler_params=pltpu.CompilerParams(vmem_limit_bytes=32 << 20),
        name="finish",
    )(tile, field, edge_rows, edge_cols)


def pack_kernel(owners, corners, values, out, request, taken, wide, narrow, sems_in, sems_out):
    group = SOURCES // 4

    def arrives(g):
        at = pl.ds(group * g, group)
        return pltpu.make_async_copy(values.at[at], wide.at[at], sems_in.at[g])

    def leaves(i, slot):
        return pltpu.make_async_copy(narrow.at[i], out.at[slot], sems_out.at[i])

    for g in range(4):
        arrives(g).start()
    for k in range(SOURCES):
        taken[k] = 0
    for k in range(2 * SLOTS):
        request[k] = 0
    slots = []
    for i in range(SOURCES):
        rank = taken[owners[i]]
        taken[owners[i]] = rank + 1
        slot = owners[i] * CAP + rank
        request[2 * slot] = corners[2 * i] + 1
        request[2 * slot + 1] = corners[2 * i + 1] + 1
        slots.append(slot)
    for i in range(SOURCES):
        if i % group == 0:
            arrives(i // group).wait()
        narrow[i] = wide[i].astype(BF16)
        leaves(i, slots[i]).start()
    for i in range(SOURCES):
        leaves(i, slots[i]).wait()


def pack_call(owners, corners, intensities):
    return pl.pallas_call(
        pack_kernel,
        out_shape=(
            jax.ShapeDtypeStruct((SLOTS, N, N), BF16),
            jax.ShapeDtypeStruct((2 * SLOTS,), jnp.int32),
        ),
        in_specs=[SMEM, SMEM, HBM],
        out_specs=(HBM, SMEM),
        scratch_shapes=[
            pltpu.SMEM((SOURCES,), jnp.int32),
            pltpu.VMEM((SOURCES, N, N), F32),
            pltpu.VMEM((SOURCES, N, N), BF16),
            pltpu.SemaphoreType.DMA((4,)),
            pltpu.SemaphoreType.DMA((SOURCES,)),
        ],
        compiler_params=pltpu.CompilerParams(vmem_limit_bytes=57 << 20),
        name="pack",
    )(owners, corners, intensities)


def moved(x, axis, step):
    size = lax.axis_size(axis)
    return lax.ppermute(x, axis, [(i, (i + step) % size) for i in range(size)])


def rows_around(edge_rows, edge_cols):
    above, below = moved(edge_rows[4:], BATCH, 1), moved(edge_rows[:4], BATCH, -1)
    for_left = jnp.concatenate([edge_cols[:4], jnp.broadcast_to(above[:, :1], (4, 128))], 1)
    for_right = jnp.concatenate([edge_cols[4:], jnp.broadcast_to(below[:, -1:], (4, 128))], 1)
    return jnp.concatenate([above, below]), for_left, for_right


def cols_around(for_left, for_right):
    return jnp.concatenate([moved(for_left, TILE, -1), moved(for_right, TILE, 1)])


def summed_shares(shares):
    shares = lax.all_to_all(shares, BATCH_TILE, split_axis=0, concat_axis=0, tiled=True)
    mine = jnp.sum(shares.astype(F32), 0, keepdims=True).astype(BF16)
    return jnp.broadcast_to(mine, shares.shape)


def from_all(mine):
    total = lax.all_to_all(mine, BATCH_TILE, split_axis=0, concat_axis=0, tiled=True)
    return total.astype(F32).reshape(2, 2, N, 128).transpose(0, 2, 1, 3).reshape(2, N, N)


def on_device(object_field, probe_wave, intensities, owner_rows, offsets):
    nbatch = lax.axis_size(BATCH)
    sent, request = pack_call(owner_rows.reshape(-1), offsets.reshape(-1), intensities)
    sent, request = lax.optimization_barrier((sent, request))
    wanted = lax.all_to_all(
        request.reshape(nbatch, CAP * 2), BATCH, split_axis=0, concat_axis=0, tiled=True
    ).reshape(SLOTS * 2)
    sent, wanted = lax.optimization_barrier((sent.reshape(nbatch, CAP, N, N), wanted))
    ints = lax.all_to_all(sent, BATCH, split_axis=0, concat_axis=0, tiled=True)
    ints = ints.reshape(SLOTS, N, N)
    exits, psi, edge_rows, edge_cols = forward_call(wanted, object_field, probe_wave)
    rows, *columns = rows_around(edge_rows, edge_cols)
    wanted, columns = lax.optimization_barrier((wanted, columns))
    columns = cols_around(*columns)
    field_grad, probe_shares = backward_call(wanted, object_field, probe_wave, ints, exits, psi)
    mine = summed_shares(probe_shares)
    new_object = finish_call(object_field, field_grad, rows, columns)
    mine, new_object = lax.optimization_barrier((mine, new_object))
    probe_total = from_all(mine)
    new_probe = probe_wave.astype(F32) - probe_rate * probe_total
    return (new_object, new_probe)


def solution(mesh):
    finer = Mesh(mesh.devices.reshape(4, 4, 4, 2), ("batch_0", "batch_1", "tile_0", "tile_1"))
    placed = (P(None, None, BATCH, TILE), P(), P(BATCH_TILE), P(BATCH_TILE), P(BATCH_TILE))
    return jax.shard_map(
        on_device,
        mesh=finer,
        in_specs=placed,
        out_specs=(P(None, None, BATCH, TILE), P()),
        check_vma=False,
    )
```

```python
import jax
import jax.numpy as jnp
import numpy as np
from jax import lax
from jax.experimental import pallas as pl
from jax.experimental.pallas import tpu as pltpu
from jax.sharding import Mesh
from jax.sharding import PartitionSpec as P

BATCH = ("batch_0", "batch_1")
TILE = ("tile_0", "tile_1")
BATCH_TILE = BATCH + TILE

update_rate = 0.1
tv_weight = 12.0
tv_smooth = 1.0
probe_rate = 0.04

N = 256
T = 384
CAP = 2
R = 32
PIECES = N // R
F32 = jnp.float32
BF16 = jnp.bfloat16


def tables():
    counter = np.arange(N)
    angles = (counter[:, None] * counter[None, :] % N) * (2.0 * np.pi / N)
    cos_table = (np.cos(angles) / np.sqrt(N)).astype(jnp.bfloat16)
    sin_table = (-np.sin(angles) / np.sqrt(N)).astype(jnp.bfloat16)
    freq = (counter + N // 2) % N - N // 2
    squared = (freq * freq).astype(np.float64)
    phases = -(0.5 / N) * (squared[:, None] + squared[None, :])
    prop = np.stack([np.cos(phases), np.sin(phases)]).astype(np.float32)
    return np.stack([cos_table, sin_table, -sin_table]), prop, halves(cos_table, sin_table)


def halves(cos_table, sin_table):
    out = []
    for sin in (sin_table, -sin_table):
        for odd in range(2):
            c, d = cos_table[: N // 2, odd::2], sin[: N // 2, odd::2]
            out.append(np.block([[c, -d], [d, c]]))
    return np.stack(out)


def rows(j):
    return pl.ds(R * j, R)


def issue(acc, regs, pushes, lhs):
    for step in range(2):
        for q in range(2):
            pltpu.matmul_push_rhs(pushes[q][step], staging_register=regs[step], mxu_index=q)
        for j in range(PIECES):
            for q in range(2):
                pltpu.matmul_acc_lhs(
                    acc[q][j], lhs[q][step](j), load_staged_rhs=regs[step] if j == 0 else None
                )


def shared(start, acc, x, y, tab, half):
    row, col = start
    regs = (0, 1)
    lane = lax.broadcasted_iota(jnp.int32, (R, 128), 1)
    back = (128 - col) & 127
    forth = col & 127
    keep = lane < 128 - col
    moved = lane >= col

    def left(forward):
        for odd in range(2):
            part = [
                jnp.concatenate([x[q, c, pl.ds(odd, N // 2, stride=2), :] for c in range(2)], 1)
                for q in range(2)
            ]
            pltpu.matmul_push_rhs(
                jnp.concatenate(part, 0).astype(BF16), staging_register=0, mxu_index=odd
            )
        for j in range(PIECES):
            for odd in range(2):
                lhs = half[(0 if forward else 2) + odd, rows(j)]
                pltpu.matmul_acc_lhs(acc[odd][j], lhs, load_staged_rhs=0 if j == 0 else None)

    def middle():
        for j in range(PIECES // 2):
            for q in range(2):
                even = pltpu.matmul_pop(acc[0][PIECES // 2 * q + j])
                odd = pltpu.matmul_pop(acc[1][PIECES // 2 * q + j])
                y[q][rows(j)] = (even + odd).astype(BF16)
                y[q][rows(PIECES // 2 + j)] = (even - odd).astype(BF16)

    def keep_x(q, j, value):
        for c in range(2):
            x[q, c, rows(j)] = value[:, 128 * c : 128 * c + 128]

    def right(forward):
        sin, neg = (1, 2) if forward else (2, 1)
        lhs = (lambda j: y[0][rows(j)], lambda j: y[1][rows(j)])
        issue(acc, regs, ((tab[0], tab[neg]), (tab[sin], tab[0])), (lhs, lhs))

    def pops(j):
        return pltpu.matmul_pop(acc[0][j]), pltpu.matmul_pop(acc[1][j])

    def cut(tile, s, q, j):
        at = pl.ds(row + R * j, R)
        turned = [pltpu.roll(tile[s, q, k, at, :], back, 1) for k in range(3)]
        return jnp.concatenate(
            [jnp.where(keep, turned[0], turned[1]), jnp.where(keep, turned[1], turned[2])], 1
        )

    def put(field, s, q, j, value):
        value = value.astype(BF16).astype(F32)
        turned = [pltpu.roll(value[:, 128 * k : 128 * k + 128], forth, 1) for k in range(2)]
        parts = (
            jnp.where(moved, turned[0], 0.0),
            jnp.where(moved, turned[1], turned[0]),
            jnp.where(moved, 0.0, turned[1]),
        )
        at = pl.ds(row + R * j, R)
        for k in range(3):
            field[s, q, k, at, :] = field[s, q, k, at, :] + parts[k]

    def kick(prop, sign):
        for j in range(PIECES):
            fr, fi = pops(j)
            hr, hi = prop[0, rows(j)], prop[1, rows(j)]
            if sign > 0:
                keep_x(0, j, hr * fr - hi * fi)
                keep_x(1, j, hr * fi + hi * fr)
            else:
                keep_x(0, j, hr * fr + hi * fi)
                keep_x(1, j, hr * fi - hi * fr)

    return left, middle, right, pops, cut, put, kick, keep_x


def forward_steps(env, start, acc, x, y, psi, exits):
    tile, probe, tab, prop, half = env
    left, middle, right, pops, cut, _, kick, keep_x = shared(start, acc, x, y, tab, half)
    for j in range(PIECES):
        tr, ti = cut(tile, 0, 0, j), cut(tile, 0, 1, j)
        pr, pi = probe[0, rows(j)].astype(F32), probe[1, rows(j)].astype(F32)
        keep_x(0, j, pr * tr - pi * ti)
        keep_x(1, j, pr * ti + pi * tr)
    left(True)
    yield
    middle()
    right(True)
    yield
    kick(prop, 1)
    left(False)
    yield
    middle()
    right(False)
    yield
    for j in range(PIECES):
        wr, wi = pops(j)
        wr, wi = wr.astype(BF16), wi.astype(BF16)
        psi[0, rows(j)] = wr
        psi[1, rows(j)] = wi
        wr, wi = wr.astype(F32), wi.astype(F32)
        tr, ti = cut(tile, 1, 0, j), cut(tile, 1, 1, j)
        keep_x(0, j, wr * tr - wi * ti)
        keep_x(1, j, wr * ti + wi * tr)
    left(True)
    yield
    middle()
    right(True)
    yield
    for j in range(PIECES):
        er, ei = pops(j)
        exits[0, rows(j)] = er
        exits[1, rows(j)] = ei


def backward_steps(env, start, scale, ints, acc, x, y, psi, exits, field):
    tile, probe, tab, prop, half, probe_sum = env
    left, middle, right, pops, cut, put, kick, keep_x = shared(start, acc, x, y, tab, half)
    for j in range(PIECES):
        er, ei = exits[0, rows(j)], exits[1, rows(j)]
        misfit = scale * (er * er + ei * ei - ints[rows(j)].astype(F32))
        keep_x(0, j, misfit * er)
        keep_x(1, j, misfit * ei)
    left(False)
    yield
    middle()
    right(False)
    yield
    for j in range(PIECES):
        gr, gi = pops(j)
        wr, wi = psi[0, rows(j)].astype(F32), psi[1, rows(j)].astype(F32)
        tr, ti = cut(tile, 1, 0, j), cut(tile, 1, 1, j)
        keep_x(0, j, gr * tr + gi * ti)
        keep_x(1, j, gi * tr - gr * ti)
        put(field, 1, 0, j, gr * wr + gi * wi)
        put(field, 1, 1, j, gi * wr - gr * wi)
    left(False)
    yield
    middle()
    right(False)
    yield
    kick(prop, -1)
    left(True)
    yield
    middle()
    right(True)
    yield
    for j in range(PIECES):
        gr, gi = pops(j)
        wr, wi = probe[0, rows(j)].astype(F32), probe[1, rows(j)].astype(F32)
        tr, ti = cut(tile, 0, 0, j), cut(tile, 0, 1, j)
        probe_sum[0, rows(j)] = probe_sum[0, rows(j)] + (gr * tr + gi * ti)
        probe_sum[1, rows(j)] = probe_sum[1, rows(j)] + (gi * tr - gr * ti)
        put(field, 0, 0, j, gr * wr + gi * wi)
        put(field, 0, 1, j, gi * wr - gr * wi)


def interleave(*steps):
    live = list(steps)
    while live:
        for one in list(live):
            if next(one, 1) == 1:
                live.remove(one)


def list_used(wanted, listed):
    def one(k, used):
        listed[used] = k
        return used + (wanted[2 * k] > 0).astype(jnp.int32)

    return lax.fori_loop(0, SLOTS, one, jnp.int32(0))


def chosen(wanted, listed, count, pair):
    there = 2 * pair + 1 < count
    slots = listed[2 * pair], listed[jnp.where(there, 2 * pair + 1, 2 * pair)]
    return slots, [(wanted[2 * k] - 1, wanted[2 * k + 1] - 1) for k in slots], there


def round_tile(tile_in, tile):
    for s in range(2):
        for q in range(2):
            for k in range(3):
                tile[s, q, k] = tile_in[s, q, :, pl.ds(128 * k, 128)].astype(BF16).astype(F32)


def with_accumulators(body):
    def start(acc_a, acc_b):
        for one in acc_a + acc_b:
            for ref in one:
                pltpu.matmul_pop(ref)
        body(acc_a, acc_b)

    refs = tuple(tuple(pltpu.ACC(q)((R, N), F32) for _ in range(PIECES)) for q in range(2))
    pl.run_scoped(start, refs, refs)


def forward_kernel(
    wanted, tile_in, probe, tab, prop, half, exits_out, psi_out, edge_rows, edge_cols, tile, listed, x, y, exits, psi, sems
):
    round_tile(tile_in, tile)
    for s in range(2):
        for q in range(2):
            k = 2 * s + q
            edge_rows[k : k + 1] = tile_in[s, q, 0:1, :]
            edge_rows[4 + k : 5 + k] = tile_in[s, q, T - 1 : T, :]
            edge_cols[k : k + 1] = jnp.transpose(tile_in[s, q, :, 0:128])[0:1]
            edge_cols[4 + k : 5 + k] = jnp.transpose(tile_in[s, q, :, T - 128 : T])[127:128]
    env = (tile, probe, tab, prop, half)
    count = list_used(wanted, listed)
    pairs = (count + 1) // 2

    def copies(b, at):
        return (
            pltpu.make_async_copy(exits.at[b], exits_out.at[at], sems.at[0, b]),
            pltpu.make_async_copy(psi.at[b], psi_out.at[at], sems.at[1, b]),
        )

    def body(acc_a, acc_b):
        @pl.loop(0, pairs)
        def _(pair):
            b = pair % 2
            _, at, _ = chosen(wanted, listed, count, pair)

            @pl.when(pair >= 2)
            def _():
                for one in copies(b, pair - 2):
                    one.wait()

            interleave(
                *[
                    forward_steps(
                        env,
                        at[i],
                        (acc_a, acc_b)[i],
                        x.at[i],
                        (y.at[i, 0], y.at[i, 1]),
                        psi.at[b, i],
                        exits.at[b, i],
                    )
                    for i in range(2)
                ]
            )
            for one in copies(b, pair):
                one.start()

        for late in (2, 1):

            @pl.when(pairs >= late)
            def _():
                for one in copies((pairs - late) % 2, pairs - late):
                    one.wait()

    with_accumulators(body)


def backward_kernel(
    wanted, tile_in, probe, tab, prop, half, ints, exits_in, psi_in, field_out, probe_out, *scratch
):
    tile, field_a, field_b, probe_sum, listed, x, y, exits, psi, sems = scratch
    count = list_used(wanted, listed)
    pairs = (count + 1) // 2

    def copies(b, at):
        return (
            pltpu.make_async_copy(exits_in.at[at], exits.at[b], sems.at[0, b]),
            pltpu.make_async_copy(psi_in.at[at], psi.at[b], sems.at[1, b]),
        )

    @pl.when(pairs > 0)
    def _():
        for one in copies(0, 0):
            one.start()

    round_tile(tile_in, tile)
    for field in (field_a, field_b):
        for s in range(2):
            for q in range(2):
                for k in range(3):
                    field[s, q, k] = jnp.zeros((T, 128), F32)
    probe_sum[...] = jnp.zeros((2, N, N), F32)
    env = (tile, probe, tab, prop, half, probe_sum)

    def body(acc_a, acc_b):
        @pl.loop(0, pairs)
        def _(pair):
            b = pair % 2
            slots, at, there = chosen(wanted, listed, count, pair)

            @pl.when(pair + 1 < pairs)
            def _():
                for one in copies(1 - b, pair + 1):
                    one.start()

            for one in copies(b, pair):
                one.wait()
            scales = F32(0.5), jnp.where(there, F32(0.5), F32(0.0))
            interleave(
                *[
                    backward_steps(
                        env,
                        at[i],
                        scales[i],
                        ints.at[slots[i]],
                        (acc_a, acc_b)[i],
                        x.at[i],
                        (y.at[i, 0], y.at[i, 1]),
                        psi.at[b, i],
                        exits.at[b, i],
                        (field_a, field_b)[i],
                    )
                    for i in range(2)
                ]
            )

    with_accumulators(body)
    for s in range(2):
        for q in range(2):
            for k in range(3):
                field_out[s, q, :, pl.ds(128 * k, 128)] = field_a[s, q, k] + field_b[s, q, k]
    for q in range(2):
        for c in range(2):
            for j in range(N // 8):
                share = probe_sum[q, 8 * j : 8 * j + 8, 128 * c : 128 * c + 128]
                probe_out[SHARES // 2 * q + N // 8 * c + j] = share.astype(BF16)


def finish_kernel(tile, field, edge_rows, edge_cols, out, padded, flow_y, flow_x, flat):
    flat[...] = jnp.zeros((128, 512), F32)
    flat[0:8] = edge_cols[...]
    tall = jnp.transpose(flat[...])
    for s in range(2):
        for q in range(2):
            k = 2 * s + q
            for block, side in ((0, 4 + k), (4, k)):
                values = jnp.broadcast_to(tall[: T + 8, side : side + 1], (T + 8, 128))
                padded[s, q, block, 8 : 8 + T] = values[:T]
                padded[s, q, block, 0:8] = values[T:]
                padded[s, q, block, 8 + T : 16 + T] = values[T:]
            for c in range(3):
                at = slice(128 * c, 128 * c + 128)
                padded[s, q, 1 + c, 8 : 8 + T] = tile[s, q, :, at]
                padded[s, q, 1 + c, 0:8] = jnp.broadcast_to(edge_rows[k : k + 1, at], (8, 128))
                padded[s, q, 1 + c, 8 + T : 16 + T] = jnp.broadcast_to(
                    edge_rows[4 + k : 5 + k, at], (8, 128)
                )
    high = 56
    lane = lax.broadcasted_iota(jnp.int32, (high, 128), 1)
    for s in range(2):
        for at in range(0, T + 8, high):
            for c in range(4):
                dy, dx = [], []
                for q in range(2):
                    here = padded[s, q, c, at : at + high]
                    after = padded[s, q, c + 1, at : at + high]
                    dy.append(padded[s, q, c, at + 1 : at + 1 + high] - here)
                    right = jnp.where(lane == 127, pltpu.roll(after, 127, 1), pltpu.roll(here, 127, 1))
                    dx.append(right - here)
                total = dy[0] * dy[0] + dx[0] * dx[0] + (dy[1] * dy[1] + dx[1] * dx[1])
                m = lax.rsqrt(total + tv_smooth)
                for q in range(2):
                    flow_y[s, q, c, at : at + high] = m * dy[q]
                    flow_x[s, q, c, at : at + high] = m * dx[q]
    high = 64
    lane = lax.broadcasted_iota(jnp.int32, (high, 128), 1)
    for s in range(2):
        for q in range(2):
            for at in range(0, T, high):
                for c in range(1, 4):
                    low = at + 8
                    down = flow_y[s, q, c, low : low + high]
                    above = flow_y[s, q, c, low - 1 : low - 1 + high]
                    right = flow_x[s, q, c, low : low + high]
                    before = flow_x[s, q, c - 1, low : low + high]
                    left = jnp.where(lane == 0, pltpu.roll(before, 1, 1), pltpu.roll(right, 1, 1))
                    to = slice(128 * c - 128, 128 * c)
                    grad = field[s, q, at : at + high, to] + tv_weight * (above + left - down - right)
                    out[s, q, at : at + high, to] = padded[s, q, c, low : low + high] - update_rate * grad


VMEM = pl.BlockSpec(memory_space=pltpu.VMEM)
SMEM = pl.BlockSpec(memory_space=pltpu.SMEM)
HBM = pl.BlockSpec(memory_space=pltpu.HBM)
SOURCES = 16
SLOTS = SOURCES * CAP
PAIRS = SLOTS // 2
SHARES = 2 * N * N // (8 * 128)
WIDE = pltpu.VMEM((2, 2, 3, T, 128), F32)
TWO = pltpu.VMEM((2, 2, N, N), BF16)
FRONTS = [
    pltpu.VMEM((2, 2, 2, N, N), F32),
    pltpu.VMEM((2, 2, 2, N, N), BF16),
    pltpu.SemaphoreType.DMA((2, 2)),
]
SPLIT = pltpu.VMEM((2, 2, 2, N, 128), F32)
LISTED = pltpu.SMEM((SLOTS + 1,), jnp.int32)


def params(limit):
    flops = SLOTS * 3 * 2 * 8 * N**3
    return dict(
        compiler_params=pltpu.CompilerParams(vmem_limit_bytes=limit << 20),
        cost_estimate=pl.CostEstimate(flops=flops, transcendentals=0, bytes_accessed=32 << 20),
    )


def forward_call(wanted, tile, probe):
    tab, prop, half = tables()
    return pl.pallas_call(
        forward_kernel,
        out_shape=(
            jax.ShapeDtypeStruct((PAIRS, 2, 2, N, N), F32),
            jax.ShapeDtypeStruct((PAIRS, 2, 2, N, N), BF16),
            jax.ShapeDtypeStruct((8, T), F32),
            jax.ShapeDtypeStruct((8, T), F32),
        ),
        in_specs=[SMEM] + [VMEM] * 5,
        out_specs=(HBM, HBM, VMEM, VMEM),
        scratch_shapes=[WIDE, LISTED, SPLIT, TWO] + FRONTS,
        name="forward",
        **params(57),
    )(wanted, tile, probe, tab, prop, half)


def backward_call(wanted, tile, probe, ints, exits, psi):
    tab, prop, half = tables()
    return pl.pallas_call(
        backward_kernel,
        out_shape=(jax.ShapeDtypeStruct((2, 2, T, T), F32), jax.ShapeDtypeStruct((SHARES, 8, 128), BF16)),
        in_specs=[SMEM] + [VMEM] * 6 + [HBM, HBM],
        out_specs=(VMEM, VMEM),
        scratch_shapes=[WIDE, WIDE, WIDE, pltpu.VMEM((2, N, N), F32), LISTED, SPLIT, TWO] + FRONTS,
        name="backward",
        **params(57),
    )(wanted, tile, probe, tab, prop, half, ints, exits, psi)


def finish_call(tile, field, edge_rows, edge_cols):
    return pl.pallas_call(
        finish_kernel,
        out_shape=jax.ShapeDtypeStruct((2, 2, T, T), F32),
        in_specs=[VMEM] * 4,
        out_specs=VMEM,
        scratch_shapes=[
            pltpu.VMEM((2, 2, 5, T + 16, 128), F32),
            pltpu.VMEM((2, 2, 4, T + 8, 128), F32),
            pltpu.VMEM((2, 2, 4, T + 8, 128), F32),
            pltpu.VMEM((128, 512), F32),
        ],
        compiler_params=pltpu.CompilerParams(vmem_limit_bytes=32 << 20),
        name="finish",
    )(tile, field, edge_rows, edge_cols)


def route_kernel(owners, corners, request, slots, taken):
    for k in range(SOURCES):
        taken[k] = 0
    for k in range(2 * SLOTS):
        request[k] = 0
    for i in range(SOURCES):
        rank = taken[owners[i]]
        taken[owners[i]] = rank + 1
        slot = owners[i] * CAP + rank
        request[2 * slot] = corners[2 * i] + 1
        request[2 * slot + 1] = corners[2 * i + 1] + 1
        slots[i] = slot


def route_call(owners, corners):
    return pl.pallas_call(
        route_kernel,
        out_shape=(
            jax.ShapeDtypeStruct((2 * SLOTS,), jnp.int32),
            jax.ShapeDtypeStruct((SOURCES,), jnp.int32),
        ),
        in_specs=[SMEM, SMEM],
        out_specs=(SMEM, SMEM),
        scratch_shapes=[pltpu.SMEM((SOURCES,), jnp.int32)],
        name="route",
    )(owners, corners)


def pack_kernel(slots, values, out, wide, narrow, sems_in, sems_out):
    group = SOURCES // 4

    def arrives(g):
        at = pl.ds(group * g, group)
        return pltpu.make_async_copy(values.at[at], wide.at[at], sems_in.at[g])

    def leaves(i):
        return pltpu.make_async_copy(narrow.at[i], out.at[slots[i]], sems_out.at[i])

    for g in range(4):
        arrives(g).start()
    for i in range(SOURCES):
        if i % group == 0:
            arrives(i // group).wait()
        narrow[i] = wide[i].astype(BF16)
        leaves(i).start()
    for i in range(SOURCES):
        leaves(i).wait()


def pack_call(slots, intensities):
    return pl.pallas_call(
        pack_kernel,
        out_shape=jax.ShapeDtypeStruct((SLOTS, N, N), BF16),
        in_specs=[SMEM, HBM],
        out_specs=HBM,
        scratch_shapes=[
            pltpu.VMEM((SOURCES, N, N), F32),
            pltpu.VMEM((SOURCES, N, N), BF16),
            pltpu.SemaphoreType.DMA((4,)),
            pltpu.SemaphoreType.DMA((SOURCES,)),
        ],
        compiler_params=pltpu.CompilerParams(vmem_limit_bytes=57 << 20),
        name="pack",
    )(slots, intensities)


def moved(x, axis, step):
    size = lax.axis_size(axis)
    return lax.ppermute(x, axis, [(i, (i + step) % size) for i in range(size)])


def rows_around(edge_rows, edge_cols):
    above, below = moved(edge_rows[4:], BATCH, 1), moved(edge_rows[:4], BATCH, -1)
    for_left = jnp.concatenate([edge_cols[:4], jnp.broadcast_to(above[:, :1], (4, 128))], 1)
    for_right = jnp.concatenate([edge_cols[4:], jnp.broadcast_to(below[:, -1:], (4, 128))], 1)
    return jnp.concatenate([above, below]), for_left, for_right


def cols_around(for_left, for_right):
    return jnp.concatenate([moved(for_left, TILE, -1), moved(for_right, TILE, 1)])


def summed_shares(shares):
    shares = lax.all_to_all(shares, BATCH_TILE, split_axis=0, concat_axis=0, tiled=True)
    mine = jnp.sum(shares.astype(F32), 0, keepdims=True).astype(BF16)
    return jnp.broadcast_to(mine, shares.shape)


def from_all(mine):
    total = lax.all_to_all(mine, BATCH_TILE, split_axis=0, concat_axis=0, tiled=True)
    return total.astype(F32).reshape(2, 2, N, 128).transpose(0, 2, 1, 3).reshape(2, N, N)


def on_device(object_field, probe_wave, intensities, owner_rows, offsets):
    nbatch = lax.axis_size(BATCH)
    request, slots = route_call(owner_rows.reshape(-1), offsets.reshape(-1))
    wanted = lax.all_to_all(
        request.reshape(nbatch, CAP * 2), BATCH, split_axis=0, concat_axis=0, tiled=True
    ).reshape(SLOTS * 2)
    sent = pack_call(slots, intensities).reshape(nbatch, CAP, N, N)
    ints = lax.all_to_all(sent, BATCH, split_axis=0, concat_axis=0, tiled=True)
    ints = ints.reshape(SLOTS, N, N)
    exits, psi, edge_rows, edge_cols = forward_call(wanted, object_field, probe_wave)
    rows, *columns = rows_around(edge_rows, edge_cols)
    wanted, columns = lax.optimization_barrier((wanted, columns))
    columns = cols_around(*columns)
    field_grad, probe_shares = backward_call(wanted, object_field, probe_wave, ints, exits, psi)
    mine = summed_shares(probe_shares)
    new_object = finish_call(object_field, field_grad, rows, columns)
    mine, new_object = lax.optimization_barrier((mine, new_object))
    probe_total = from_all(mine)
    new_probe = probe_wave.astype(F32) - probe_rate * probe_total
    return (new_object, new_probe)


def solution(mesh):
    finer = Mesh(mesh.devices.reshape(4, 4, 4, 2), ("batch_0", "batch_1", "tile_0", "tile_1"))
    placed = (P(None, None, BATCH, TILE), P(), P(BATCH_TILE), P(BATCH_TILE), P(BATCH_TILE))
    return jax.shard_map(
        on_device,
        mesh=finer,
        in_specs=placed,
        out_specs=(P(None, None, BATCH, TILE), P()),
        check_vma=False,
    )
```
